32 devices in a mesh: gx: 8 (over z, x), gy: 4 (over y, core).
Axes of the slice: x: 2, y: 2, z: 4, core: 2. Of those that a mesh axis runs over, the one named last changes fastest.
Arguments:
- right_side: float32 [3, 224, 12432], P(None, 'gx', 'gy'), may hold values from -6 to 6
- guess: float32 [3, 224, 12432], P(None, 'gx', 'gy'), may hold values from -6 to 6
- material: int32 [32, 16, 16], P('gx', 'gy'), may hold values from 0 to 7
- lame: float32 [2, 8], replicated, may hold values from 0.5 to 2
- upper: float32 [1], replicated, may hold values from 3 to 6
- lower_ratio: float32 [1], replicated, may hold values from 0.05 to 0.3
Outputs:
- smoothed: float32 [3, 224, 12432], P(None, 'gx', 'gy')
- residual: float32 [3, 224, 12432], P(None, 'gx', 'gy')
The draws below stay inside these ranges and needn't reach their ends.
All inputs are finite; a program needn't handle non-finite values.
Results may differ from the reference program's by a relative error of at most 0.0003.
Values sent between devices are 32-bit elements; how exact they have to be, the bound alone decides.
A program may use at most 128 MiB of HBM per device.

```python
import math
import jax
import jax.numpy as jnp
import numpy as np
from jax import lax

DEG = 7
EZ = 16
NMAT = 8
SWEEPS = 2
CHEB = 3
NEX = 32
NEY = 16
NXN = 224
NYN = 112
ZN = 111


def plant(entries, rng, smallest, largest):
    dims = entries.shape
    place = [jax.random.randint(jax.random.fold_in(rng, axis), (), 0, dims[axis]) for axis in range(len(dims))]
    entries = entries.at[tuple(place)].set(smallest)
    longest = dims.index(max(dims))
    place[longest] = (place[longest] + 1) % dims[longest]
    return entries.at[tuple(place)].set(largest)


def block_levels(own_key, dims, split, low, largest):
    loudness = 1.0
    for axis_at, parts in split:
        heights = jax.random.uniform(jax.random.fold_in(jax.random.fold_in(own_key, 6), axis_at), (parts,), jnp.float32, low / len(split), largest / len(split))
        loudness = loudness * jnp.repeat(jnp.exp(heights), dims[axis_at] // parts).reshape((-1,) + (1,) * (len(dims) - 1 - axis_at))
    return loudness


def normal_values(own_key, shape, spread, most, cuts=(), kind=jnp.bfloat16):
    drawn = spread * jax.random.normal(own_key, shape, jnp.float32)
    if cuts:
        drawn = drawn * block_levels(own_key, shape, cuts, -0.22, 0.18)
    return jnp.clip(drawn, -most, most).astype(kind)


def setup_inputs(seed: int = 0) -> dict:
    seeds = jax.random.split(jax.random.key(seed), 7)
    return {
        "right_side": normal_values(seeds[0], (3, NXN, NYN * ZN), 0.5, 6.0, ((1, 8), (2, 4)), jnp.float32),
        "guess": normal_values(seeds[1], (3, NXN, NYN * ZN), 1.0, 6.0, ((1, 8), (2, 4)), jnp.float32),
        "material": plant(jax.random.randint(seeds[2], (NEX, NEY, EZ), 0, NMAT), jax.random.fold_in(seeds[2], 1), 0, NMAT - 1).astype(jnp.int32),
        "lame": jnp.clip(jnp.exp(jax.random.uniform(seeds[3], (2, NMAT), jnp.float32, math.log(0.5), math.log(2.0))), 0.5, 2.0),
        "upper": jnp.clip(jax.random.uniform(seeds[4], (1,), jnp.float32, 3.0, 6.0), 3.0, 6.0),
        "lower_ratio": jnp.clip(jax.random.uniform(seeds[5], (1,), jnp.float32, 0.05, 0.3), 0.05, 0.3),
    }


highest = lax.Precision.HIGHEST


def legendre_pair(points, degree):
    prev_poly = points * 0.0 + 1.0
    this_poly = points * 1.0
    for order in range(2, degree + 1):
        next_poly = ((2 * order - 1) * points * this_poly - (order - 1) * prev_poly) / order
        prev_poly = this_poly
        this_poly = next_poly
    return this_poly, prev_poly


def gll_tables(degree):
    count = degree + 1
    points = -np.cos(np.pi * np.arange(count) / degree)
    for newton_step in range(60):
        this_poly, prev_poly = legendre_pair(points, degree)
        points = points - (points * this_poly - prev_poly) / (count * this_poly)
    values, unused_poly = legendre_pair(points, degree)
    weights = 2.0 / (degree * (degree + 1) * values ** 2)
    identity_np = np.eye(count)
    spacing = points[:, None] - points[None, :] + identity_np
    derivative = values[:, None] / (values[None, :] * spacing) * (1.0 - identity_np)
    derivative[0, 0] = -degree * (degree + 1) / 4.0
    derivative[degree, degree] = degree * (degree + 1) / 4.0
    stiff_ratio = (weights[:, None] * derivative ** 2).sum(0) / weights
    return weights, derivative, stiff_ratio


def split_periodic(field_in, dim_index):
    layout = field_in.shape
    blocks = layout[dim_index] // DEG
    leading = field_in.reshape(layout[:dim_index] + (blocks, DEG) + layout[dim_index + 1:])
    first_node = lax.slice_in_dim(leading, 0, 1, axis=dim_index + 1)
    return jnp.concatenate([leading, jnp.roll(first_node, -1, axis=dim_index)], axis=dim_index + 1)


def fold_periodic(element_vals, dim_index):
    layout = element_vals.shape
    blocks = layout[dim_index]
    leading = lax.slice_in_dim(element_vals, 0, DEG, axis=dim_index + 1)
    trailing = lax.slice_in_dim(element_vals, DEG, DEG + 1, axis=dim_index + 1)
    first_node = lax.slice_in_dim(leading, 0, 1, axis=dim_index + 1) + jnp.roll(trailing, 1, axis=dim_index)
    remaining = lax.slice_in_dim(leading, 1, DEG, axis=dim_index + 1)
    joined = jnp.concatenate([first_node, remaining], axis=dim_index + 1)
    return joined.reshape(layout[:dim_index] + (blocks * DEG,) + layout[dim_index + 2:])


def split_clamped(field_in):
    layout = field_in.shape
    blocks = (layout[-1] + 1) // DEG
    widths = [(0, 0)] * (len(layout) - 1) + [(1, 1)]
    padded = jnp.pad(field_in, widths)
    leading = padded[..., :blocks * DEG].reshape(layout[:-1] + (blocks, DEG))
    trailing = padded[..., DEG::DEG][..., None]
    joined = jnp.concatenate([leading, trailing], -1)
    return joined.reshape(layout[:-1] + (blocks * (DEG + 1),))


def fold_clamped(element_vals):
    layout = element_vals.shape
    blocks = layout[-1] // (DEG + 1)
    split_vals = element_vals.reshape(layout[:-1] + (blocks, DEG + 1))
    leading = split_vals[..., :DEG].reshape(layout[:-1] + (blocks * DEG,))
    trailing = split_vals[..., DEG:]
    filler = jnp.zeros(layout[:-1] + (blocks, DEG - 1), element_vals.dtype)
    spread_tail = jnp.concatenate([filler, trailing], -1).reshape(layout[:-1] + (blocks * DEG,))
    no_pad = [(0, 0)] * (len(layout) - 1)
    full_line = jnp.pad(leading, no_pad + [(0, 1)]) + jnp.pad(spread_tail, no_pad + [(1, 0)])
    return full_line[..., 1:blocks * DEG]


def along_z(field_in, matrix):
    layout = field_in.shape
    split_vals = field_in.reshape(layout[:-1] + (layout[-1] // (DEG + 1), DEG + 1))
    return jnp.einsum('pk,...k->...p', matrix, split_vals, precision=highest).reshape(layout)


def element_forces(element_vals, lam_w, mu_w, derivative, z_grad, z_back):
    grad_x = jnp.einsum('pi,cxiyjz->cxpyjz', derivative, element_vals, precision=highest)
    grad_y = jnp.einsum('pj,cxiyjz->cxiypz', derivative, element_vals, precision=highest)
    grad_z = along_z(element_vals, z_grad)
    gradients = jnp.stack([grad_x, grad_y, grad_z])
    divergence = gradients[0, 0] + gradients[1, 1] + gradients[2, 2]
    identity = jnp.eye(3, dtype=jnp.float32).reshape(3, 3, 1, 1, 1, 1, 1)
    stress = mu_w * (gradients + jnp.swapaxes(gradients, 0, 1)) + lam_w * divergence * identity
    forces = jnp.einsum('pi,cxpyjz->cxiyjz', derivative, stress[0], precision=highest)
    forces = forces + jnp.einsum('pj,cxiypz->cxiyjz', derivative, stress[1], precision=highest)
    return forces + along_z(stress[2], z_back)


def element_diagonal(lam_w, mu_w, ratio_x, ratio_y, ratio_z):
    ratio_sum = ratio_x + ratio_y + ratio_z
    pieces = [lam_w * own_ratio + mu_w * (ratio_sum + own_ratio) for own_ratio in (ratio_x, ratio_y, ratio_z)]
    return jnp.stack(pieces)


def point_weight(weights, blocks_z):
    weights_z = jnp.tile(weights, blocks_z)
    return weights[None, :, None, None, None] * weights[None, None, None, :, None] * weights_z[None, None, None, None, :]


def point_coeffs(lam_el, mu_el, point_w):
    lam_rep = jnp.repeat(lam_el, DEG + 1, axis=2)[:, None, :, None, :]
    mu_rep = jnp.repeat(mu_el, DEG + 1, axis=2)[:, None, :, None, :]
    return lam_rep * point_w, mu_rep * point_w


def lame_fields(material, lame):
    labels = jnp.arange(lame.shape[1], dtype=jnp.int32)
    onehot = (material[..., None] == labels).astype(jnp.float32)
    coeffs = jnp.einsum('xyzm,km->kxyz', onehot, lame, precision=highest)
    return coeffs[0], coeffs[1]


def assemble_slabs(results):
    return fold_clamped(fold_periodic(jnp.moveaxis(results, 0, 1), 1))


def reference(right_side, guess, material, lame, upper, lower_ratio):
    weights_np, derivative_np, ratio_np = gll_tables(DEG)
    weights = jnp.asarray(weights_np, dtype=jnp.float32)
    derivative = jnp.asarray(derivative_np, dtype=jnp.float32)
    stiff_ratio = jnp.asarray(ratio_np, dtype=jnp.float32)
    point_w = point_weight(weights, EZ)
    ratio_x = stiff_ratio.reshape(1, DEG + 1, 1, 1, 1)
    ratio_y = stiff_ratio.reshape(1, 1, 1, DEG + 1, 1)
    ratio_z = jnp.tile(stiff_ratio, EZ).reshape(1, 1, 1, 1, -1)
    lam_el, mu_el = lame_fields(material, lame)
    shape_four = (3, NXN, NYN, ZN)
    source = right_side.reshape(shape_four)
    solution = guess.reshape(shape_four)

    def operate(field_in):
        slabs = jnp.moveaxis(split_periodic(split_clamped(field_in), 1), 1, 0)

        def one_slab(inputs):
            column_slab, lam_slab, mu_slab = inputs
            lam_w, mu_w = point_coeffs(lam_slab[None], mu_slab[None], point_w)
            element_vals = split_periodic(column_slab, 2)[:, None]
            forces = element_forces(element_vals, lam_w, mu_w, derivative, derivative, derivative.T)
            return fold_periodic(forces[:, 0], 2)

        return assemble_slabs(lax.map(one_slab, (slabs, lam_el, mu_el)))

    def diag_slab(inputs):
        lam_slab, mu_slab = inputs
        lam_w, mu_w = point_coeffs(lam_slab[None], mu_slab[None], point_w)
        pieces = element_diagonal(lam_w, mu_w, ratio_x, ratio_y, ratio_z)
        return fold_periodic(pieces[:, 0], 2)

    diagonal = assemble_slabs(lax.map(diag_slab, (lam_el, mu_el)))
    inverse = 1.0 / diagonal
    upper_edge = upper[0]
    lower_edge = lower_ratio[0] * upper_edge
    center = (upper_edge + lower_edge) / 2.0
    radius = (upper_edge - lower_edge) / 2.0
    sigma_ratio = center / radius
    for sweep_index in range(SWEEPS):
        residual = source - operate(solution)
        change = inverse * residual / center
        solution = solution + change
        factor = 1.0 / sigma_ratio
        for step_index in range(CHEB - 1):
            factor_next = 1.0 / (2.0 * sigma_ratio - factor)
            residual = source - operate(solution)
            change = factor_next * factor * change + (2.0 * factor_next / radius) * inverse * residual
            solution = solution + change
            factor = factor_next
    residual = source - operate(solution)
    flat_shape = (3, NXN, NYN * ZN)
    return solution.reshape(flat_shape), residual.reshape(flat_shape)
```

```python
import jax
import jax.numpy as jnp
import numpy as np
from jax import lax
from jax.experimental import pallas as pl
from jax.experimental.pallas import tpu as pltpu
from jax.sharding import PartitionSpec as P

DEG = 7
SWEEPS = 2
CHEB = 3


highest = lax.Precision.HIGHEST


def legendre_pair(points, degree):
    prev_poly = points * 0.0 + 1.0
    this_poly = points * 1.0
    for order in range(2, degree + 1):
        next_poly = ((2 * order - 1) * points * this_poly - (order - 1) * prev_poly) / order
        prev_poly = this_poly
        this_poly = next_poly
    return (this_poly, prev_poly)


def gll_tables(degree):
    count = degree + 1
    points = -np.cos(np.pi * np.arange(count) / degree)
    for newton_step in range(60):
        this_poly, prev_poly = legendre_pair(points, degree)
        points = points - (points * this_poly - prev_poly) / (count * this_poly)
    values, unused_poly = legendre_pair(points, degree)
    weights = 2.0 / (degree * (degree + 1) * values**2)
    identity_np = np.eye(count)
    spacing = points[:, None] - points[None, :] + identity_np
    derivative = values[:, None] / (values[None, :] * spacing) * (1.0 - identity_np)
    derivative[0, 0] = -degree * (degree + 1) / 4.0
    derivative[degree, degree] = degree * (degree + 1) / 4.0
    stiff_ratio = (weights[:, None] * derivative**2).sum(0) / weights
    return (weights, derivative, stiff_ratio)


def clamped_gather(blocks):
    free_nodes = DEG * blocks - 1
    selector = np.zeros((free_nodes, blocks * (DEG + 1)), np.float32)
    for element in range(blocks):
        for node_idx in range(DEG + 1):
            target = DEG * element + node_idx - 1
            if 0 <= target < free_nodes:
                selector[target, element * (DEG + 1) + node_idx] = 1.0
    return selector


N1 = DEG + 1
SLOTS = 4
UNROLL = 6


def halves(value):
    high = value.astype(jnp.bfloat16)
    low = (value - high.astype(jnp.float32)).astype(jnp.bfloat16)
    return high, low


def np_halves(matrix):
    high = np.asarray(matrix, np.float32).astype(jnp.bfloat16)
    low = (np.asarray(matrix, np.float64) - high.astype(np.float64)).astype(jnp.bfloat16)
    return high, low


def apply_pairs(matrix, values, parity):
    half = N1 // 2
    even = [values[i] + values[DEG - i] for i in range(half)]
    odd = [values[i] - values[DEG - i] for i in range(half)]
    outs = [None] * N1
    for p in range(half):
        plus = None
        minus = None
        for i in range(half):
            by_even = float(np.float32((matrix[p, i] + matrix[p, DEG - i]) / 2))
            by_odd = float(np.float32((matrix[p, i] - matrix[p, DEG - i]) / 2))
            plus = by_even * even[i] if plus is None else plus + by_even * even[i]
            minus = by_odd * odd[i] if minus is None else minus + by_odd * odd[i]
        outs[p] = minus + plus
        outs[DEG - p] = plus - minus if parity > 0 else minus - plus
    return outs


def element_tables():
    weights, derivative, ratio = gll_tables(DEG)
    own = derivative.T * weights[None, :] / weights[:, None]
    second = own @ derivative
    return weights, derivative, ratio, own, second


def smoother_kernel(
    steps,
    elems_x,
    elems_y,
    lame,
    upper,
    lower_ratio,
    guess_in,
    source_in,
    material,
    weight_in,
    own_in,
    sum_in,
    spread_in,
    gather_in,
    select_in,
    edge_in,
    own_mat,
    back_mat,
    second_mat,
    join_in,
    smoothed_out,
    residual_out,
    coef,
    field,
    resid,
    source,
    lam_w,
    mu_w,
    inverse,
    change,
    along_x,
    own_z,
    stress_x,
    part_x,
    flat_a,
    flat_b,
    send_x,
    send_y,
    send_c,
    recv_x,
    recv_y,
    recv_c,
    send_sem,
    recv_sem,
):
    cols = elems_x * elems_y
    size_x = lax.axis_size("gx")
    size_y = lax.axis_size("gy")
    me_x = lax.axis_index("gx")
    me_y = lax.axis_index("gy")
    near_x = (lax.rem(me_x + size_x - 1, size_x), lax.rem(me_x + 1, size_x))
    near_y = (lax.rem(me_y + size_y - 1, size_y), lax.rem(me_y + 1, size_y))
    partners = [(near_x[0], me_y), (near_x[1], me_y), (me_x, near_y[0]), (me_x, near_y[1])]
    partners += [(near_x[a], near_y[b]) for a in range(2) for b in range(2)]

    barrier = pltpu.get_barrier_semaphore()
    for partner in partners:
        pl.semaphore_signal(
            barrier, inc=1, device_id=partner, device_id_type=pl.DeviceIdType.MESH
        )

    def copies(slot, c):
        made = []
        for d in range(8):
            if d < 2:
                src, dst = send_x.at[slot, c, d], recv_x.at[slot, c, 1 - d]
            elif d < 4:
                src, dst = send_y.at[slot, c, d - 2], recv_y.at[slot, c, 3 - d]
            else:
                src, dst = send_c.at[slot, c, d - 4], recv_c.at[slot, c, 7 - d]
            mirror = (1, 0, 3, 2, 7, 6, 5, 4)[d]
            made.append(
                pltpu.make_async_remote_copy(
                    src_ref=src,
                    dst_ref=dst,
                    send_sem=send_sem.at[slot, c, d],
                    recv_sem=recv_sem.at[slot, c, mirror],
                    device_id=partners[d],
                    device_id_type=pl.DeviceIdType.MESH,
                )
            )
        return made

    rows = lax.broadcasted_iota(jnp.int32, (N1 * cols, 128), 0) % cols
    row_x = rows % elems_x
    inner_low_y = rows >= elems_x
    inner_high_y = rows < cols - elems_x
    inner_low_x = row_x >= 1
    inner_high_x = row_x < elems_x - 1
    last_x = elems_x - 1
    last_y = cols - elems_x
    flat = (N1 * cols, 128)
    full = (N1, cols, 128)

    def local_sum(ref, c):
        zero = jnp.zeros(flat, jnp.float32)
        low = ref[c, 0].reshape(flat)
        high = ref[c, DEG].reshape(flat)
        to_low = jnp.where(inner_low_x, pltpu.roll(high, 1, 0), zero)
        to_high = jnp.where(inner_high_x, pltpu.roll(low, N1 * cols - 1, 0), zero)
        ref[c, 0] = (low + to_low).reshape(full)
        ref[c, DEG] = (high + to_high).reshape(full)
        low = ref[c, :, 0].reshape(flat)
        high = ref[c, :, DEG].reshape(flat)
        to_low = jnp.where(inner_low_y, pltpu.roll(high, elems_x, 0), zero)
        to_high = jnp.where(inner_high_y, pltpu.roll(low, N1 * cols - elems_x, 0), zero)
        ref[c, :, 0] = (low + to_low).reshape(full)
        ref[c, :, DEG] = (high + to_high).reshape(full)

    def post(ref, slot, c):
        send_y[slot, c, 0] = ref[c, :, 0, 0:elems_x, :]
        send_y[slot, c, 1] = ref[c, :, DEG, last_y:cols, :]
        for b in range(elems_y):
            at = b * elems_x
            send_x[slot, c, 0, :, b : b + 1, :] = ref[c, 0, :, at : at + 1, :]
            at = b * elems_x + last_x
            send_x[slot, c, 1, :, b : b + 1, :] = ref[c, DEG, :, at : at + 1, :]
        for a in range(2):
            for b in range(2):
                at = a * last_x + b * last_y
                send_c[slot, c, 2 * a + b] = ref[c, a * DEG, b * DEG, at : at + 1, :]
        for copy in copies(slot, c):
            copy.start()

    def collect(ref, slot, c):
        for copy in copies(slot, c):
            copy.wait()
        ref[c, :, 0, 0:elems_x, :] += recv_y[slot, c, 0]
        ref[c, :, DEG, last_y:cols, :] += recv_y[slot, c, 1]
        for b in range(elems_y):
            at = b * elems_x
            ref[c, 0, :, at : at + 1, :] += recv_x[slot, c, 0, :, b : b + 1, :]
            at = b * elems_x + last_x
            ref[c, DEG, :, at : at + 1, :] += recv_x[slot, c, 1, :, b : b + 1, :]
        for a in range(2):
            for b in range(2):
                at = a * last_x + b * last_y
                ref[c, a * DEG, b * DEG, at : at + 1, :] += recv_c[slot, c, 2 * a + b]

    nodes_x = DEG * elems_x
    nodes_y = DEG * elems_y
    nodes_z = guess_in.shape[2] // nodes_y
    pad_x = flat_a.shape[1]
    zeros_big = jnp.zeros((N1, cols, 128), jnp.float32)

    @pl.loop(0, nodes_y)
    def _(y):
        flat_a[y] = jnp.zeros((pad_x, 128), jnp.float32)
        flat_b[y] = jnp.zeros((pad_x, 128), jnp.float32)

    def through(src, dst, matrix):
        @pl.loop(0, elems_y, unroll=elems_y)
        def _(b):
            pick = pl.ds(b * DEG, DEG)
            parts = halves(src[pick].reshape(DEG * pad_x, 128))
            dst[pick] = jnp.dot(
                jnp.concatenate(parts, axis=1), matrix[...], preferred_element_type=jnp.float32
            ).reshape(DEG, pad_x, 128)

    def enter(flat_in, ref, c):
        lines = flat_in[c]
        for y in range(nodes_y):
            flat_a[y, 0:nodes_x, 0:nodes_z] = lines[:, y * nodes_z : (y + 1) * nodes_z]
        through(flat_a, flat_b, gather_in)
        ref[c, DEG] = zeros_big
        ref[c, :, DEG] = zeros_big
        for b in range(elems_y):
            for j in range(DEG):
                for i in range(DEG):
                    ref[c, i, j, b * elems_x : (b + 1) * elems_x, :] = flat_b[
                        b * DEG + j, pl.ds(i, elems_x, stride=DEG), :
                    ]

    def leave(ref, flat_out, c):
        for b in range(elems_y):
            for j in range(DEG):
                for i in range(DEG):
                    flat_b[b * DEG + j, pl.ds(i, elems_x, stride=DEG), :] = ref[
                        c, i, j, b * elems_x : (b + 1) * elems_x, :
                    ]
        through(flat_b, flat_a, select_in)
        lines = [flat_a[y, 0:nodes_x, 0:nodes_z] for y in range(nodes_y)]
        flat_out[c] = jnp.concatenate(lines, axis=1)

    @pl.loop(0, 3)
    def _(c):
        enter(guess_in, field, c)
        local_sum(field, c)

    pl.semaphore_wait(barrier, len(partners))

    @pl.loop(0, 3)
    def _(c):
        post(field, 0, c)

    upper_edge = jnp.full((1, 128), upper[0], jnp.float32)
    lower_edge = lower_ratio[0] * upper_edge
    center = (upper_edge + lower_edge) / 2.0
    radius = (upper_edge - lower_edge) / 2.0
    sigma_ratio = center / radius
    for sweep in range(SWEEPS):
        coef[0, sweep * CHEB] = jnp.zeros((1, 128), jnp.float32)
        coef[1, sweep * CHEB] = 1.0 / center
        factor = 1.0 / sigma_ratio
        for later in range(1, CHEB):
            factor_next = 1.0 / (2.0 * sigma_ratio - factor)
            coef[0, sweep * CHEB + later] = factor_next * factor
            coef[1, sweep * CHEB + later] = 2.0 * factor_next / radius
            factor = factor_next

    kinds = jnp.concatenate([material[:, b, :] for b in range(elems_y)], axis=0)
    tables = []
    for row in range(2):
        picked = jnp.zeros(kinds.shape, jnp.float32)
        for kind in range(lame.shape[1]):
            picked = jnp.where(kinds == kind, lame[row, kind], picked)
        tables.append(
            jnp.dot(picked, spread_in[...], precision=highest, preferred_element_type=jnp.float32)
        )
    lam_all, mu_all = tables

    @pl.loop(0, N1)
    def _(i):
        for j in range(N1):
            lam_w[i, j] = lam_all * weight_in[i, j]
            mu_w[i, j] = mu_all * weight_in[i, j]

    @pl.loop(0, 3 * N1, unroll=N1)
    def _(at):
        c = at // N1
        i = at % N1
        pieces = []
        for j in range(N1):
            own = own_in[c, i, j]
            pieces.append(lam_w[i, j] * own + mu_w[i, j] * (sum_in[i, j] + own))
        high, low = halves(jnp.concatenate(pieces, axis=0))
        summed = jnp.dot(
            jnp.concatenate([high, low], axis=1), join_in[...], preferred_element_type=jnp.float32
        )
        inverse[c, i] = summed.reshape(N1, cols, 128)

    for c in range(3):
        local_sum(inverse, c)
        post(inverse, 1, c)

    weights, derivative, _, own, second = element_tables()
    edge = float(np.float32(1.0 / weights[0]))
    groups = [slice(8 * h, 8 * h + 8) for h in range(cols // 8)]

    def product(parts, matrix):
        both = jnp.dot(
            jnp.concatenate(parts, axis=1), matrix[...], preferred_element_type=jnp.float32
        )
        return (both[:, :128] + both[:, 128:]).reshape(full)

    def forward(c, j, values):
        if c == 2:
            own_z[:, j] = product(halves(values.reshape(flat)), own_mat)
        for rows in groups:
            lines = [values[i, rows] for i in range(N1)]
            outs = apply_pairs(own, lines, -1) if c == 0 else apply_pairs(second, lines, 1)
            for i in range(N1):
                along_x[c, i, j, rows] = outs[i]

    def begin(c):
        @pl.loop(0, N1, unroll=N1)
        def _(j):
            forward(c, j, field[c, :, j])

    def advance(c, step):
        alpha = coef[0, step]
        beta = coef[1, step]

        @pl.loop(0, N1, unroll=N1)
        def _(j):
            new = alpha * change[c, :, j] + beta * (inverse[c, :, j] * resid[c, :, j])
            change[c, :, j] = new
            new = field[c, :, j] + new
            field[c, :, j] = new
            forward(c, j, new)

    def sheet(i, edge_x):
        lines_y = []
        lines_v = []
        lines_z = []
        lines_t = []
        edge_z = edge_in[...]
        for rows in groups:
            u_x = [field[0, i, j, rows] for j in range(N1)]
            u_y = [field[1, i, j, rows] for j in range(N1)]
            u_z = [field[2, i, j, rows] for j in range(N1)]
            g_y = apply_pairs(own, u_y, -1)
            second_x = apply_pairs(second, u_x, 1)
            second_z = apply_pairs(second, u_z, 1)
            extra_y = []
            t_y = []
            group_v = []
            group_z = []
            group_t = []
            for j in range(N1):
                lam = lam_w[i, j, rows]
                mu = mu_w[i, j, rows]
                g_x = along_x[0, i, j, rows]
                g_z = own_z[i, j, rows]
                g_xy = g_x + g_y[j]
                total = g_xy + g_z
                e_z = edge_z * u_z[j]
                div = e_z - total
                own_x = -g_x
                own_y = -g_y[j]
                left = second_x[j]
                right = along_x[1, i, j, rows]
                if edge_x is not None:
                    e_x = edge_x * u_x[j]
                    div = div + e_x
                    own_x = (e_x + e_x) - g_x
                    left = left + edge_x * (g_y[j] + g_z)
                if j in (0, DEG):
                    edge_y = -edge if j == 0 else edge
                    e_y = edge_y * u_y[j]
                    div = div + e_y
                    own_y = (e_y + e_y) - g_y[j]
                    right = right + edge_y * (g_x + g_z)
                base = lam * div - mu * total
                stress_x[i, j, rows] = base + mu * own_x
                part_x[i, j, rows] = mu * left
                t_y.append(base + mu * own_y)
                extra_y.append(mu * right)
                group_v.append(mu * u_y[j])
                group_t.append(base + mu * ((e_z + e_z) - g_z))
                group_z.append(mu * ((along_x[2, i, j, rows] + second_z[j]) + edge_z * g_xy))
            back_y = apply_pairs(derivative.T, t_y, -1)
            lines_y.append([back_y[j] + extra_y[j] for j in range(N1)])
            lines_v.append(group_v)
            lines_z.append(group_z)
            lines_t.append(group_t)

        def stacked(lines):
            return jnp.concatenate([lines[h][j] for j in range(N1) for h in range(len(groups))], axis=0)

        parts = halves(stacked(lines_y)) + halves(stacked(lines_v))
        resid[1, i] = source[1, i] - product(parts, second_mat)
        parts = halves(stacked(lines_z)) + halves(stacked(lines_t))
        resid[2, i] = source[2, i] - product(parts, back_mat)

    def closing(j):
        lines_x = []
        lines_v = []
        for rows in groups:
            back_x = apply_pairs(derivative.T, [stress_x[i, j, rows] for i in range(N1)], -1)
            lines_x.append([part_x[i, j, rows] + back_x[i] for i in range(N1)])
            lines_v.append([mu_w[i, j, rows] * field[0, i, j, rows] for i in range(N1)])

        def stacked(lines):
            return jnp.concatenate([lines[h][i] for i in range(N1) for h in range(len(groups))], axis=0)

        parts = halves(stacked(lines_x)) + halves(stacked(lines_v))
        resid[0, :, j] = source[0, :, j] - product(parts, second_mat)

    def residuals(slot):
        @pl.loop(1, DEG, unroll=UNROLL)
        def _(i):
            sheet(i, None)

        for side in range(2):
            sheet(side * DEG, edge if side else -edge)

        @pl.loop(1, 3)
        def _(c):
            local_sum(resid, c)
            post(resid, slot, c)

        @pl.loop(0, N1, unroll=N1)
        def _(j):
            closing(j)

        local_sum(resid, 0)
        post(resid, slot, 0)

    @pl.loop(0, 3)
    def _(c):
        enter(source_in, source, c)

    for c in (1, 2, 0):
        collect(field, 0, c)
        begin(c)

    @pl.loop(0, 3)
    def _(c):
        collect(inverse, 1, c)

        @pl.loop(0, N1)
        def _(i):
            inverse[c, i] = 1.0 / inverse[c, i]
            change[c, i] = zeros_big

    @pl.loop(0, steps)
    def _(step):
        slot = 2 + step % 2
        residuals(slot)

        for c in (1, 2, 0):
            collect(resid, slot, c)
            advance(c, step)

    slot = 2 + steps % 2
    residuals(slot)

    @pl.loop(0, 3)
    def _(c):
        leave(field, smoothed_out, c)

    @pl.loop(0, 3)
    def _(c):
        collect(resid, slot, c)
        leave(resid, residual_out, c)


def z_join(blocks, clamped):
    nodes = DEG * blocks + 1
    gather = np.zeros((nodes, blocks * N1))
    for element in range(blocks):
        for k in range(N1):
            gather[DEG * element + k, element * N1 + k] = 1.0
    if clamped:
        gather[0] = 0.0
        gather[nodes - 1] = 0.0
    return gather.T @ gather


def local(right_side, guess, material, lame, upper, lower_ratio):
    elems_x, elems_y, elems_z = material.shape
    cols = elems_x * elems_y
    lanes = N1 * elems_z
    nodes_z = DEG * elems_z - 1
    weights_np, derivative_np, ratio_np, own_np_1, second_np = element_tables()
    eye_z = np.eye(elems_z)
    join_np = z_join(elems_z, True)
    joined = join_np.astype(jnp.bfloat16)

    def exact_pair(matrix):
        high, low = np_halves(matrix)
        none = np.zeros_like(high)
        return [[high, low], [high, none]]

    exact_join = [[joined, np.zeros_like(joined)]] * 2
    own_mat = jnp.asarray(np.block(exact_pair(np.kron(eye_z, own_np_1.T))))
    back_np = np.kron(eye_z, derivative_np) @ join_np
    back_mat = jnp.asarray(np.block(exact_join + exact_pair(back_np)))
    scaled_np = np.kron(eye_z, second_np) @ join_np
    second_mat = jnp.asarray(np.block(exact_join + exact_pair(scaled_np)))
    edge_np = np.zeros((1, lanes))
    edge_np[0, 0::N1] = -1.0 / weights_np[0]
    edge_np[0, DEG::N1] = 1.0 / weights_np[DEG]
    edge_in = jnp.asarray(edge_np, jnp.float32)
    all_join = z_join(elems_z, False).astype(jnp.bfloat16)
    join_in = jnp.asarray(np.concatenate([all_join, all_join], axis=0))

    weights_z = np.tile(weights_np, elems_z)
    ratio_z = np.tile(ratio_np, elems_z)
    weight_np = weights_np[:, None, None] * weights_np[None, :, None] * weights_z
    shape_w = (N1, N1, lanes)
    own_x = np.broadcast_to(ratio_np[:, None, None], shape_w)
    own_y = np.broadcast_to(ratio_np[None, :, None], shape_w)
    own_z = np.broadcast_to(ratio_z, shape_w)
    own_np = np.stack([own_x, own_y, own_z])
    weight_in = jnp.asarray(weight_np[:, :, None], jnp.float32)
    own_in = jnp.asarray(own_np[:, :, :, None], jnp.float32)
    sum_in = jnp.asarray((own_x + own_y + own_z)[:, :, None], jnp.float32)

    gather_np = clamped_gather(elems_z)
    nodes_z = gather_np.shape[0]
    owned_np = gather_np.copy()
    owned_np[:, DEG::N1] = 0.0
    enter_np = np.zeros((lanes, lanes))
    enter_np[:nodes_z] = gather_np
    leave_np = np.zeros((lanes, lanes))
    leave_np[:, :nodes_z] = owned_np.T
    gather_in = jnp.asarray(np.concatenate([enter_np, enter_np], axis=0).astype(jnp.bfloat16))
    select_in = jnp.asarray(np.concatenate([leave_np, leave_np], axis=0).astype(jnp.bfloat16))
    spread_in = jnp.asarray(np.kron(eye_z, np.ones((1, N1))), dtype=jnp.float32)

    pad_x = -(-DEG * elems_x // 8) * 8
    whole = (3, N1, N1, cols, lanes)
    vmem = pl.BlockSpec(memory_space=pltpu.VMEM)
    smem = pl.BlockSpec(memory_space=pltpu.SMEM)
    big = pltpu.VMEM(whole, jnp.float32)
    small = pltpu.VMEM((N1, N1, cols, lanes), jnp.float32)
    lines = pltpu.VMEM((DEG * elems_y, pad_x, lanes), jnp.float32)
    face_x = pltpu.VMEM((SLOTS, 3, 2, N1, elems_y, lanes), jnp.float32)
    face_y = pltpu.VMEM((SLOTS, 3, 2, N1, elems_x, lanes), jnp.float32)
    corner = pltpu.VMEM((SLOTS, 3, 4, 1, lanes), jnp.float32)
    shape = jax.ShapeDtypeStruct(guess.shape, jnp.float32)

    def kernel(*refs):
        smoother_kernel(SWEEPS * CHEB, elems_x, elems_y, *refs)

    return pl.pallas_call(
        kernel,
        out_shape=(shape, shape),
        in_specs=[smem] * 3 + [vmem] * 14,
        out_specs=(vmem, vmem),
        scratch_shapes=[pltpu.VMEM((2, SWEEPS * CHEB, 1, lanes), jnp.float32)]
        + [big] * 3
        + [small] * 2
        + [big] * 3
        + [small] * 3
        + [lines] * 2
        + [face_x, face_y, corner] * 2
        + [pltpu.SemaphoreType.DMA((SLOTS, 3, 8))] * 2,
        compiler_params=pltpu.CompilerParams(collective_id=0, has_side_effects=True),
    )(
        lame,
        upper,
        lower_ratio,
        guess,
        right_side,
        material,
        weight_in,
        own_in,
        sum_in,
        spread_in,
        gather_in,
        select_in,
        edge_in,
        own_mat,
        back_mat,
        second_mat,
        join_in,
    )


def solution(mesh):
    placed = (P(None, "gx", "gy"), P(None, "gx", "gy"), P("gx", "gy", None), P(), P(), P())
    return jax.shard_map(
        local,
        mesh=mesh,
        in_specs=placed,
        out_specs=(P(None, "gx", "gy"), P(None, "gx", "gy")),
        check_vma=False,
    )
```

```python
import jax
import jax.numpy as jnp
import numpy as np
from jax import lax
from jax.experimental import pallas as pl
from jax.experimental.pallas import tpu as pltpu
from jax.sharding import PartitionSpec as P

DEG = 7
SWEEPS = 2
CHEB = 3


highest = lax.Precision.HIGHEST


def legendre_pair(points, degree):
    prev_poly = points * 0.0 + 1.0
    this_poly = points * 1.0
    for order in range(2, degree + 1):
        next_poly = ((2 * order - 1) * points * this_poly - (order - 1) * prev_poly) / order
        prev_poly = this_poly
        this_poly = next_poly
    return (this_poly, prev_poly)


def gll_tables(degree):
    count = degree + 1
    points = -np.cos(np.pi * np.arange(count) / degree)
    for newton_step in range(60):
        this_poly, prev_poly = legendre_pair(points, degree)
        points = points - (points * this_poly - prev_poly) / (count * this_poly)
    values, unused_poly = legendre_pair(points, degree)
    weights = 2.0 / (degree * (degree + 1) * values**2)
    identity_np = np.eye(count)
    spacing = points[:, None] - points[None, :] + identity_np
    derivative = values[:, None] / (values[None, :] * spacing) * (1.0 - identity_np)
    derivative[0, 0] = -degree * (degree + 1) / 4.0
    derivative[degree, degree] = degree * (degree + 1) / 4.0
    stiff_ratio = (weights[:, None] * derivative**2).sum(0) / weights
    return (weights, derivative, stiff_ratio)


def clamped_gather(blocks):
    free_nodes = DEG * blocks - 1
    selector = np.zeros((free_nodes, blocks * (DEG + 1)), np.float32)
    for element in range(blocks):
        for node_idx in range(DEG + 1):
            target = DEG * element + node_idx - 1
            if 0 <= target < free_nodes:
                selector[target, element * (DEG + 1) + node_idx] = 1.0
    return selector


N1 = DEG + 1
SLOTS = 3
UNROLL = 6


def halves(value):
    high = value.astype(jnp.bfloat16)
    low = (value - high.astype(jnp.float32)).astype(jnp.bfloat16)
    return high, low


def np_halves(matrix):
    high = np.asarray(matrix, np.float32).astype(jnp.bfloat16)
    low = (np.asarray(matrix, np.float64) - high.astype(np.float64)).astype(jnp.bfloat16)
    return high, low


def apply_pairs(matrix, values, parity):
    half = N1 // 2
    even = [values[i] + values[DEG - i] for i in range(half)]
    odd = [values[i] - values[DEG - i] for i in range(half)]
    outs = [None] * N1
    for p in range(half):
        plus = None
        minus = None
        for i in range(half):
            by_even = float(np.float32((matrix[p, i] + matrix[p, DEG - i]) / 2))
            by_odd = float(np.float32((matrix[p, i] - matrix[p, DEG - i]) / 2))
            plus = by_even * even[i] if plus is None else plus + by_even * even[i]
            minus = by_odd * odd[i] if minus is None else minus + by_odd * odd[i]
        outs[p] = minus + plus
        outs[DEG - p] = plus - minus if parity > 0 else minus - plus
    return outs


def element_tables():
    weights, derivative, ratio = gll_tables(DEG)
    own = derivative.T * weights[None, :] / weights[:, None]
    second = own @ derivative
    return weights, derivative, ratio, own, second


def smoother_kernel(
    steps,
    elems_x,
    elems_y,
    lame,
    upper,
    lower_ratio,
    guess_in,
    source_in,
    material,
    weight_in,
    own_in,
    sum_in,
    spread_in,
    gather_in,
    select_in,
    edge_in,
    own_mat,
    back_mat,
    second_mat,
    exact_mat,
    join_in,
    smoothed_out,
    residual_out,
    coef,
    field,
    resid,
    source,
    lam_w,
    mu_w,
    inverse,
    change,
    along_x,
    own_z,
    stress_x,
    part_x,
    arrived,
    scale,
    rank,
    flat_a,
    flat_b,
    send_x,
    send_y,
    send_c,
    recv_x,
    recv_y,
    recv_c,
    send_sem,
    recv_sem,
):
    cols = elems_x * elems_y
    size_x = lax.axis_size("gx")
    size_y = lax.axis_size("gy")
    me_x = lax.axis_index("gx")
    me_y = lax.axis_index("gy")
    near_x = (lax.rem(me_x + size_x - 1, size_x), lax.rem(me_x + 1, size_x))
    near_y = (lax.rem(me_y + size_y - 1, size_y), lax.rem(me_y + 1, size_y))
    partners = [(near_x[0], me_y), (near_x[1], me_y), (me_x, near_y[0]), (me_x, near_y[1])]
    partners += [(near_x[a], near_y[b]) for a in range(2) for b in range(2)]

    barrier = pltpu.get_barrier_semaphore()
    for partner in partners:
        pl.semaphore_signal(
            barrier, inc=1, device_id=partner, device_id_type=pl.DeviceIdType.MESH
        )

    def copies(slot, c):
        made = []
        for d in range(8):
            if d < 2:
                src, dst = send_x.at[slot, c, d], recv_x.at[slot, c, 1 - d]
            elif d < 4:
                src, dst = send_y.at[slot, c, d - 2], recv_y.at[slot, c, 3 - d]
            else:
                src, dst = send_c.at[slot, c, d - 4], recv_c.at[slot, c, 7 - d]
            mirror = (1, 0, 3, 2, 7, 6, 5, 4)[d]
            made.append(
                pltpu.make_async_remote_copy(
                    src_ref=src,
                    dst_ref=dst,
                    send_sem=send_sem.at[slot, c, d],
                    recv_sem=recv_sem.at[slot, c, mirror],
                    device_id=partners[d],
                    device_id_type=pl.DeviceIdType.MESH,
                )
            )
        return made

    rows = lax.broadcasted_iota(jnp.int32, (N1 * cols, 128), 0) % cols
    row_x = rows % elems_x
    inner_low_y = rows >= elems_x
    inner_high_y = rows < cols - elems_x
    inner_low_x = row_x >= 1
    inner_high_x = row_x < elems_x - 1
    last_x = elems_x - 1
    last_y = cols - elems_x
    flat = (N1 * cols, 128)
    full = (N1, cols, 128)

    def local_sum(ref, c):
        zero = jnp.zeros(flat, jnp.float32)
        low = ref[c, 0].reshape(flat)
        high = ref[c, DEG].reshape(flat)
        to_low = jnp.where(inner_low_x, pltpu.roll(high, 1, 0), zero)
        to_high = jnp.where(inner_high_x, pltpu.roll(low, N1 * cols - 1, 0), zero)
        ref[c, 0] = (low + to_low).reshape(full)
        ref[c, DEG] = (high + to_high).reshape(full)
        low = ref[c, :, 0].reshape(flat)
        high = ref[c, :, DEG].reshape(flat)
        to_low = jnp.where(inner_low_y, pltpu.roll(high, elems_x, 0), zero)
        to_high = jnp.where(inner_high_y, pltpu.roll(low, N1 * cols - elems_x, 0), zero)
        ref[c, :, 0] = (low + to_low).reshape(full)
        ref[c, :, DEG] = (high + to_high).reshape(full)

    def post(ref, slot, c):
        send_y[slot, c, 0] = ref[c, :, 0, 0:elems_x, :]
        send_y[slot, c, 1] = ref[c, :, DEG, last_y:cols, :]
        for b in range(elems_y):
            at = b * elems_x
            send_x[slot, c, 0, :, b : b + 1, :] = ref[c, 0, :, at : at + 1, :]
            at = b * elems_x + last_x
            send_x[slot, c, 1, :, b : b + 1, :] = ref[c, DEG, :, at : at + 1, :]
        for a in range(2):
            for b in range(2):
                at = a * last_x + b * last_y
                send_c[slot, c, 2 * a + b] = ref[c, a * DEG, b * DEG, at : at + 1, :]
        for copy in copies(slot, c):
            copy.start()

    def collect(ref, slot, c):
        for copy in copies(slot, c):
            copy.wait()
        ref[c, :, 0, 0:elems_x, :] += recv_y[slot, c, 0]
        ref[c, :, DEG, last_y:cols, :] += recv_y[slot, c, 1]
        for b in range(elems_y):
            at = b * elems_x
            ref[c, 0, :, at : at + 1, :] += recv_x[slot, c, 0, :, b : b + 1, :]
            at = b * elems_x + last_x
            ref[c, DEG, :, at : at + 1, :] += recv_x[slot, c, 1, :, b : b + 1, :]
        for a in range(2):
            for b in range(2):
                at = a * last_x + b * last_y
                ref[c, a * DEG, b * DEG, at : at + 1, :] += recv_c[slot, c, 2 * a + b]

    nodes_x = DEG * elems_x
    nodes_y = DEG * elems_y
    nodes_z = guess_in.shape[2] // nodes_y
    pad_x = flat_a.shape[1]
    zeros_big = jnp.zeros((N1, cols, 128), jnp.float32)

    @pl.loop(0, nodes_y)
    def _(y):
        flat_a[y] = jnp.zeros((pad_x, 128), jnp.float32)
        flat_b[y] = jnp.zeros((pad_x, 128), jnp.float32)

    def through(src, dst, matrix):
        @pl.loop(0, elems_y, unroll=elems_y)
        def _(b):
            pick = pl.ds(b * DEG, DEG)
            parts = halves(src[pick].reshape(DEG * pad_x, 128))
            dst[pick] = jnp.dot(
                jnp.concatenate(parts, axis=1), matrix[...], preferred_element_type=jnp.float32
            ).reshape(DEG, pad_x, 128)

    def enter(flat_in, ref, c):
        lines = flat_in[c]
        for y in range(nodes_y):
            flat_a[y, 0:nodes_x, 0:nodes_z] = lines[:, y * nodes_z : (y + 1) * nodes_z]
        through(flat_a, flat_b, gather_in)
        ref[c, DEG] = zeros_big
        ref[c, :, DEG] = zeros_big
        for b in range(elems_y):
            for j in range(DEG):
                for i in range(DEG):
                    ref[c, i, j, b * elems_x : (b + 1) * elems_x, :] = flat_b[
                        b * DEG + j, pl.ds(i, elems_x, stride=DEG), :
                    ]

    def leave(ref, flat_out, c):
        for b in range(elems_y):
            for j in range(DEG):
                for i in range(DEG):
                    flat_b[b * DEG + j, pl.ds(i, elems_x, stride=DEG), :] = ref[
                        c, i, j, b * elems_x : (b + 1) * elems_x, :
                    ]
        through(flat_b, flat_a, select_in)
        lines = [flat_a[y, 0:nodes_x, 0:nodes_z] for y in range(nodes_y)]
        flat_out[c] = jnp.concatenate(lines, axis=1)

    @pl.loop(0, 3)
    def _(c):
        enter(guess_in, field, c)
        local_sum(field, c)

    pl.semaphore_wait(barrier, len(partners))

    @pl.loop(0, 3)
    def _(c):
        post(field, 0, c)

    upper_edge = jnp.full((1, 128), upper[0], jnp.float32)
    lower_edge = lower_ratio[0] * upper_edge
    center = (upper_edge + lower_edge) / 2.0
    radius = (upper_edge - lower_edge) / 2.0
    sigma_ratio = center / radius
    none_row = jnp.zeros((1, 128), jnp.float32)
    one_row = jnp.ones((1, 128), jnp.float32)
    coef[0, 0] = none_row
    coef[1, 0] = none_row
    coef[2, 0] = one_row
    for sweep in range(SWEEPS):
        first = sweep * CHEB + 1
        coef[0, first] = none_row
        coef[1, first] = 1.0 / center
        coef[2, first] = none_row
        factor = 1.0 / sigma_ratio
        for later in range(1, CHEB):
            factor_next = 1.0 / (2.0 * sigma_ratio - factor)
            coef[0, first + later] = factor_next * factor
            coef[1, first + later] = 2.0 * factor_next / radius
            coef[2, first + later] = none_row
            factor = factor_next

    kinds = jnp.concatenate([material[:, b, :] for b in range(elems_y)], axis=0)
    tables = []
    for row in range(2):
        picked = jnp.zeros(kinds.shape, jnp.float32)
        for kind in range(lame.shape[1]):
            picked = jnp.where(kinds == kind, lame[row, kind], picked)
        tables.append(
            jnp.dot(picked, spread_in[...], precision=highest, preferred_element_type=jnp.float32)
        )
    lam_all, mu_all = tables

    @pl.loop(0, N1)
    def _(i):
        for j in range(N1):
            lam_w[i, j] = lam_all * weight_in[i, j]
            mu_w[i, j] = mu_all * weight_in[i, j]

    @pl.loop(0, 3 * N1, unroll=N1)
    def _(at):
        c = at // N1
        i = at % N1
        pieces = []
        for j in range(N1):
            own = own_in[c, i, j]
            pieces.append(lam_w[i, j] * own + mu_w[i, j] * (sum_in[i, j] + own))
        high, low = halves(jnp.concatenate(pieces, axis=0))
        summed = jnp.dot(
            jnp.concatenate([high, low], axis=1), join_in[...], preferred_element_type=jnp.float32
        )
        inverse[c, i] = summed.reshape(N1, cols, 128)

    for c in range(3):
        local_sum(inverse, c)
        post(inverse, 2, c)

    weights, derivative, _, own, second = element_tables()
    edge = float(np.float32(1.0 / weights[0]))
    groups = [slice(8 * h, 8 * h + 8) for h in range(cols // 8)]

    def product(parts, matrix):
        both = jnp.dot(
            jnp.concatenate(parts, axis=1), matrix[...], preferred_element_type=jnp.float32
        )
        return (both[:, :128] + both[:, 128:]).reshape(full)

    def joint(parts, matrix):
        both = jnp.dot(
            jnp.concatenate(parts, axis=1), matrix[...], preferred_element_type=jnp.float32
        )
        return (both[:, :128] + both[:, 128:]).reshape(2, N1, cols, 128)

    def forward(c, j, values):
        if c == 2:
            own_z[:, j] = product(halves(values.reshape(flat)), own_mat)
        for rows in groups:
            lines = [values[i, rows] for i in range(N1)]
            outs = apply_pairs(own, lines, -1) if c == 0 else apply_pairs(second, lines, 1)
            for i in range(N1):
                along_x[c, i, j, rows] = outs[i]

    def advance(c, step):
        alpha = coef[0, step]
        beta = coef[1, step]

        @pl.loop(0, N1, unroll=N1)
        def _(j):
            new = alpha * change[c, :, j] + beta * (inverse[c, :, j] * resid[c, :, j])
            change[c, :, j] = new
            new = field[c, :, j] + new
            field[c, :, j] = new
            forward(c, j, new)

    def sheet(i, edge_x):
        lines_y = []
        lines_v = []
        lines_z = []
        lines_t = []
        edge_z = edge_in[...]
        for rows in groups:
            u_x = [field[0, i, j, rows] for j in range(N1)]
            u_y = [field[1, i, j, rows] for j in range(N1)]
            u_z = [field[2, i, j, rows] for j in range(N1)]
            g_y = apply_pairs(own, u_y, -1)
            second_x = apply_pairs(second, u_x, 1)
            second_z = apply_pairs(second, u_z, 1)
            extra_y = []
            t_y = []
            group_v = []
            group_z = []
            group_t = []
            for j in range(N1):
                lam = lam_w[i, j, rows]
                mu = mu_w[i, j, rows]
                g_x = along_x[0, i, j, rows]
                g_z = own_z[i, j, rows]
                g_xy = g_x + g_y[j]
                total = g_xy + g_z
                e_z = edge_z * u_z[j]
                div = e_z - total
                own_x = -g_x
                own_y = -g_y[j]
                left = second_x[j]
                right = along_x[1, i, j, rows]
                if edge_x is not None:
                    e_x = edge_x * u_x[j]
                    div = div + e_x
                    own_x = (e_x + e_x) - g_x
                    left = left + edge_x * (g_y[j] + g_z)
                if j in (0, DEG):
                    edge_y = -edge if j == 0 else edge
                    e_y = edge_y * u_y[j]
                    div = div + e_y
                    own_y = (e_y + e_y) - g_y[j]
                    right = right + edge_y * (g_x + g_z)
                base = lam * div - mu * total
                stress_x[i, j, rows] = base + mu * own_x
                part_x[i, j, rows] = mu * left
                t_y.append(base + mu * own_y)
                extra_y.append(mu * right)
                group_v.append(mu * u_y[j])
                group_t.append(base + mu * ((e_z + e_z) - g_z))
                group_z.append(mu * ((along_x[2, i, j, rows] + second_z[j]) + edge_z * g_xy))
            back_y = apply_pairs(derivative.T, t_y, -1)
            lines_y.append([back_y[j] + extra_y[j] for j in range(N1)])
            lines_v.append(group_v)
            lines_z.append(group_z)
            lines_t.append(group_t)

        def stacked(lines):
            return jnp.concatenate([lines[h][j] for j in range(N1) for h in range(len(groups))], axis=0)

        parts = halves(stacked(lines_y)) + halves(stacked(lines_v))
        resid[1, i] = source[1, i] - product(parts, second_mat)
        parts = halves(stacked(lines_z)) + halves(stacked(lines_t))
        resid[2, i] = source[2, i] - product(parts, back_mat)

    def closing(j):
        lines_x = []
        lines_v = []
        for rows in groups:
            back_x = apply_pairs(derivative.T, [stress_x[i, j, rows] for i in range(N1)], -1)
            lines_x.append([part_x[i, j, rows] + back_x[i] for i in range(N1)])
            lines_v.append([mu_w[i, j, rows] * field[0, i, j, rows] for i in range(N1)])

        def stacked(lines):
            return jnp.concatenate([lines[h][i] for i in range(N1) for h in range(len(groups))], axis=0)

        parts = halves(stacked(lines_x)) + halves(stacked(lines_v))
        resid[0, :, j] = source[0, :, j] - product(parts, second_mat)

    def volume(step):
        for c in (1, 2, 0):
            advance(c, step)

        @pl.loop(1, DEG, unroll=UNROLL)
        def _(i):
            sheet(i, None)

        for side in range(2):
            sheet(side * DEG, edge if side else -edge)

        @pl.loop(0, N1, unroll=N1)
        def _(j):
            closing(j)

    row_id = lax.broadcasted_iota(jnp.int32, (cols, 128), 0)
    col_x = row_id % elems_x
    low_side = (col_x == 0, row_id < elems_x)
    high_side = (col_x == last_x, row_id >= last_y)

    def by_side(axis, low, high):
        zero = jnp.zeros((cols, 128), jnp.float32)
        return jnp.where(low_side[axis], low, jnp.where(high_side[axis], high, zero))

    def rank_tables():
        for axis in range(2):
            for p in range(N1):
                rows = []
                for f in (0, DEG):
                    others = [k for k in range(N1) if k != f]
                    chain = sum(derivative[k, p] * weights[k] * own[k, f] for k in others)
                    away = 0.0 if p == f else weights[p]
                    rows.append((derivative[f, p], -chain, away * second[p, f], away * own[p, f]))
                for kind in range(4):
                    low, high = (float(np.float32(row[kind])) for row in rows)
                    rank[axis, kind, p] = by_side(axis, low, high)

    def spot(ref, axis, c, p, t):
        return ref.at[c, p, t] if axis == 0 else ref.at[c, t, p]

    def face_scales():
        for axis in range(2):
            for c in range(3):
                for t in range(N1):
                    scale[axis, c, t] = by_side(
                        axis, spot(inverse, axis, c, 0, t)[...], spot(inverse, axis, c, DEG, t)[...]
                    )

    def wait_for(slot, kinds):
        for c in range(3):
            made = copies(slot, c)
            for d in kinds:
                made[d].wait()

    def arrive_y(slot):
        for c in range(3):
            arrived[1, c, :, 0:elems_x, :] = recv_y[slot, c, 0]
            arrived[1, c, :, last_y:cols, :] = recv_y[slot, c, 1]

    def arrive_x(slot):
        for c in range(3):
            for b in range(elems_y):
                at = b * elems_x
                arrived[0, c, :, at : at + 1, :] = recv_x[slot, c, 0, :, b : b + 1, :]
                at = b * elems_x + last_x
                arrived[0, c, :, at : at + 1, :] = recv_x[slot, c, 1, :, b : b + 1, :]
            for a in range(2):
                for b in range(2):
                    at = a * last_x + b * last_y
                    arrived[0, c, b * DEG, at : at + 1, :] += (
                        recv_c[slot, c, 2 * a + b] + recv_y[slot, c, b, a * DEG, a * last_x : a * last_x + 1, :]
                    )

    def correct(axis, step):
        normal, side = axis, 1 - axis
        beta = coef[1, step]
        plain = coef[2, step]
        edge_z = edge_in[...]
        edge_n = by_side(axis, -edge, edge)
        own_f = by_side(axis, float(np.float32(own[0, 0])), float(np.float32(own[DEG, DEG])))
        second_f = float(np.float32(second[0, 0]))
        per_w = float(np.float32(1.0 / weights[0]))
        d = [[None] * N1 for _ in range(3)]
        for c in range(3):
            for t in range(N1):
                value = (plain + beta * scale[axis, c, t]) * arrived[axis, c, t]
                value = jnp.where(low_side[axis] | high_side[axis], value, 0.0)
                if axis == 1 and t in (0, DEG):
                    value = jnp.where(col_x == (0 if t == 0 else last_x), 0.0, value)
                d[c][t] = value
                at_low = jnp.where(low_side[axis], value, 0.0)
                at_high = jnp.where(high_side[axis], value, 0.0)
                for ref in (field, change):
                    low = spot(ref, axis, c, 0, t)
                    high = spot(ref, axis, c, DEG, t)
                    low[...] = low[...] + at_low
                    high[...] = high[...] + at_high
        d_n, d_t, d_z = d[normal], d[side], d[2]

        def stack(lines):
            return jnp.concatenate(lines, axis=0)

        g_z = product(halves(stack(d_z)), own_mat)
        g_t = apply_pairs(own, d_t, -1)
        second_n = apply_pairs(second, d_n, 1)
        second_z = apply_pairs(second, d_z, 1)
        t_n, t_t, t_z, left, v_n, v_t, extra, f_z = [[] for _ in range(8)]
        stiff, mixed, mixed_t, mixed_z, one_t, one_z = [[] for _ in range(6)]
        for t in range(N1):
            lam = lam_w[0, t]
            mu = mu_w[0, t]
            g_n = own_f * d_n[t]
            g_nt = g_n + g_t[t]
            total = g_nt + g_z[t]
            e_n = edge_n * d_n[t]
            e_z = edge_z * d_z[t]
            div = (e_n + e_z) - total
            own_t = g_t[t]
            right = second_f * d_t[t]
            lam_in = per_w * lam
            mu_in = per_w * mu
            mu_d = mu_in * d_n[t]
            mixed.append((lam_in + mu_in) * d_n[t])
            stiff.append(mixed[t] + mu_d)
            if t in (0, DEG):
                edge_t = -edge if t == 0 else edge
                e_t = edge_t * d_t[t]
                div = div + e_t
                own_t = own_t - (e_t + e_t)
                right = right + edge_t * (g_n + g_z[t])
                mixed_t.append(edge_t * mu_d)
            else:
                mixed_t.append(None)
            base = lam * div - mu * total
            t_n.append(base + mu * ((e_n + e_n) - g_n))
            t_t.append(base - mu * own_t)
            t_z.append(base + mu * ((e_z + e_z) - g_z[t]))
            left.append(mu * (second_n[t] + edge_n * (g_t[t] + g_z[t])))
            v_n.append(mu * d_n[t])
            v_t.append(mu * d_t[t])
            extra.append(mu * right)
            f_z.append(mu * ((second_f * d_z[t] + second_z[t]) + edge_z * g_nt))
            mixed_z.append(edge_z * mu_d)
            one_t.append(mu_in * d_t[t])
            one_z.append(mu_in * d_z[t])
        back_t = apply_pairs(derivative.T, t_t, -1)
        back_m = apply_pairs(-derivative.T, mixed, -1)
        f_t = [back_t[t] + extra[t] for t in range(N1)]
        two_t = [back_m[t] if mixed_t[t] is None else back_m[t] + mixed_t[t] for t in range(N1)]
        minus = [-m for m in mixed]
        joined = jnp.dot(
            jnp.concatenate(halves(stack(t_n + stiff + one_t + two_t + one_z)), axis=1),
            exact_mat[...],
            preferred_element_type=jnp.float32,
        ).reshape(5, N1, cols, 128)
        parts = halves(stack(left + f_t)) + halves(stack(v_n + v_t))
        faces = joint(parts, second_mat)
        parts = halves(stack(f_z + mixed_z)) + halves(stack(t_z + minus))
        upright = joint(parts, back_mat)
        at_face = {normal: faces[0], side: faces[1], 2: upright[0]}
        pairs = {
            normal: (0, joined[0], joined[1]),
            side: (2, joined[2], joined[3]),
            2: (2, joined[4], upright[1]),
        }
        for t in range(N1):
            for c in range(3):
                kind, first, second_part = pairs[c]
                for p in range(N1):
                    value = rank[axis, kind, p] * first[t] + rank[axis, kind + 1, p] * second_part[t]
                    if p == 0:
                        value = value + jnp.where(low_side[axis], at_face[c][t], 0.0)
                    if p == DEG:
                        value = value + jnp.where(high_side[axis], at_face[c][t], 0.0)
                    place = spot(resid, axis, c, p, t)
                    place[...] = place[...] - value

    @pl.loop(0, 3)
    def _(c):
        enter(source_in, source, c)

    rank_tables()

    @pl.loop(0, 2 * 3 * N1)
    def _(at):
        arrived[at // (3 * N1), (at // N1) % 3, at % N1] = jnp.zeros((cols, 128), jnp.float32)
        scale[at // (3 * N1), (at // N1) % 3, at % N1] = jnp.zeros((cols, 128), jnp.float32)

    @pl.loop(0, 3 * N1)
    def _(at):
        change[at // N1, at % N1] = zeros_big
        resid[at // N1, at % N1] = zeros_big

    @pl.loop(0, steps + 1)
    def _(step):
        volume(step)

        slot = step % 2
        wait_for(slot, (2, 3))
        arrive_y(slot)
        correct(1, step)
        wait_for(slot, (0, 1, 4, 5, 6, 7))
        arrive_x(slot)
        correct(0, step)

        @pl.loop(0, 3)
        def _(c):
            local_sum(resid, c)
            post(resid, 1 - slot, c)

        @pl.when(step == 0)
        def _():
            @pl.loop(0, 3)
            def _(c):
                collect(inverse, 2, c)

                @pl.loop(0, N1)
                def _(i):
                    inverse[c, i] = 1.0 / inverse[c, i]

            face_scales()

    @pl.loop(0, 3)
    def _(c):
        leave(field, smoothed_out, c)

    slot = (steps + 1) % 2

    @pl.loop(0, 3)
    def _(c):
        collect(resid, slot, c)
        leave(resid, residual_out, c)


def z_join(blocks, clamped):
    nodes = DEG * blocks + 1
    gather = np.zeros((nodes, blocks * N1))
    for element in range(blocks):
        for k in range(N1):
            gather[DEG * element + k, element * N1 + k] = 1.0
    if clamped:
        gather[0] = 0.0
        gather[nodes - 1] = 0.0
    return gather.T @ gather


def local(right_side, guess, material, lame, upper, lower_ratio):
    elems_x, elems_y, elems_z = material.shape
    cols = elems_x * elems_y
    lanes = N1 * elems_z
    nodes_z = DEG * elems_z - 1
    weights_np, derivative_np, ratio_np, own_np_1, second_np = element_tables()
    eye_z = np.eye(elems_z)
    join_np = z_join(elems_z, True)
    joined = join_np.astype(jnp.bfloat16)

    def exact_pair(matrix):
        high, low = np_halves(matrix)
        none = np.zeros_like(high)
        return [[high, low], [high, none]]

    exact_join = [[joined, np.zeros_like(joined)]] * 2
    own_mat = jnp.asarray(np.block(exact_pair(np.kron(eye_z, own_np_1.T))))
    back_np = np.kron(eye_z, derivative_np) @ join_np
    back_mat = jnp.asarray(np.block(exact_join + exact_pair(back_np)))
    scaled_np = np.kron(eye_z, second_np) @ join_np
    second_mat = jnp.asarray(np.block(exact_join + exact_pair(scaled_np)))
    exact_mat = jnp.asarray(np.concatenate([joined, joined], axis=0))
    edge_np = np.zeros((1, lanes))
    edge_np[0, 0::N1] = -1.0 / weights_np[0]
    edge_np[0, DEG::N1] = 1.0 / weights_np[DEG]
    edge_in = jnp.asarray(edge_np, jnp.float32)
    all_join = z_join(elems_z, False).astype(jnp.bfloat16)
    join_in = jnp.asarray(np.concatenate([all_join, all_join], axis=0))

    weights_z = np.tile(weights_np, elems_z)
    ratio_z = np.tile(ratio_np, elems_z)
    weight_np = weights_np[:, None, None] * weights_np[None, :, None] * weights_z
    shape_w = (N1, N1, lanes)
    own_x = np.broadcast_to(ratio_np[:, None, None], shape_w)
    own_y = np.broadcast_to(ratio_np[None, :, None], shape_w)
    own_z = np.broadcast_to(ratio_z, shape_w)
    own_np = np.stack([own_x, own_y, own_z])
    weight_in = jnp.asarray(weight_np[:, :, None], jnp.float32)
    own_in = jnp.asarray(own_np[:, :, :, None], jnp.float32)
    sum_in = jnp.asarray((own_x + own_y + own_z)[:, :, None], jnp.float32)

    gather_np = clamped_gather(elems_z)
    nodes_z = gather_np.shape[0]
    owned_np = gather_np.copy()
    owned_np[:, DEG::N1] = 0.0
    enter_np = np.zeros((lanes, lanes))
    enter_np[:nodes_z] = gather_np
    leave_np = np.zeros((lanes, lanes))
    leave_np[:, :nodes_z] = owned_np.T
    gather_in = jnp.asarray(np.concatenate([enter_np, enter_np], axis=0).astype(jnp.bfloat16))
    select_in = jnp.asarray(np.concatenate([leave_np, leave_np], axis=0).astype(jnp.bfloat16))
    spread_in = jnp.asarray(np.kron(eye_z, np.ones((1, N1))), dtype=jnp.float32)

    pad_x = -(-DEG * elems_x // 8) * 8
    whole = (3, N1, N1, cols, lanes)
    vmem = pl.BlockSpec(memory_space=pltpu.VMEM)
    smem = pl.BlockSpec(memory_space=pltpu.SMEM)
    big = pltpu.VMEM(whole, jnp.float32)
    small = pltpu.VMEM((N1, N1, cols, lanes), jnp.float32)
    face = pltpu.VMEM((2, 3, N1, cols, lanes), jnp.float32)
    lines = pltpu.VMEM((DEG * elems_y, pad_x, lanes), jnp.float32)
    face_x = pltpu.VMEM((SLOTS, 3, 2, N1, elems_y, lanes), jnp.float32)
    face_y = pltpu.VMEM((SLOTS, 3, 2, N1, elems_x, lanes), jnp.float32)
    corner = pltpu.VMEM((SLOTS, 3, 4, 1, lanes), jnp.float32)
    shape = jax.ShapeDtypeStruct(guess.shape, jnp.float32)

    def kernel(*refs):
        smoother_kernel(SWEEPS * CHEB, elems_x, elems_y, *refs)

    return pl.pallas_call(
        kernel,
        out_shape=(shape, shape),
        in_specs=[smem] * 3 + [vmem] * 15,
        out_specs=(vmem, vmem),
        scratch_shapes=[pltpu.VMEM((3, SWEEPS * CHEB + 1, 1, lanes), jnp.float32)]
        + [big] * 3
        + [small] * 2
        + [big] * 3
        + [small] * 3
        + [face] * 2
        + [pltpu.VMEM((2, 4, N1, cols, lanes), jnp.float32)]
        + [lines] * 2
        + [face_x, face_y, corner] * 2
        + [pltpu.SemaphoreType.DMA((SLOTS, 3, 8))] * 2,
        compiler_params=pltpu.CompilerParams(collective_id=0, has_side_effects=True),
    )(
        lame,
        upper,
        lower_ratio,
        guess,
        right_side,
        material,
        weight_in,
        own_in,
        sum_in,
        spread_in,
        gather_in,
        select_in,
        edge_in,
        own_mat,
        back_mat,
        second_mat,
        exact_mat,
        join_in,
    )


def solution(mesh):
    placed = (P(None, "gx", "gy"), P(None, "gx", "gy"), P("gx", "gy", None), P(), P(), P())
    return jax.shard_map(
        local,
        mesh=mesh,
        in_specs=placed,
        out_specs=(P(None, "gx", "gy"), P(None, "gx", "gy")),
        check_vma=False,
    )
```

```python
import jax
import jax.numpy as jnp
import numpy as np
from jax import lax
from jax.experimental import pallas as pl
from jax.experimental.pallas import tpu as pltpu
from jax.sharding import PartitionSpec as P

DEG = 7
SWEEPS = 2
CHEB = 3


highest = lax.Precision.HIGHEST


def legendre_pair(points, degree):
    prev_poly = points * 0.0 + 1.0
    this_poly = points * 1.0
    for order in range(2, degree + 1):
        next_poly = ((2 * order - 1) * points * this_poly - (order - 1) * prev_poly) / order
        prev_poly = this_poly
        this_poly = next_poly
    return (this_poly, prev_poly)


def gll_tables(degree):
    count = degree + 1
    points = -np.cos(np.pi * np.arange(count) / degree)
    for newton_step in range(60):
        this_poly, prev_poly = legendre_pair(points, degree)
        points = points - (points * this_poly - prev_poly) / (count * this_poly)
    values, unused_poly = legendre_pair(points, degree)
    weights = 2.0 / (degree * (degree + 1) * values**2)
    identity_np = np.eye(count)
    spacing = points[:, None] - points[None, :] + identity_np
    derivative = values[:, None] / (values[None, :] * spacing) * (1.0 - identity_np)
    derivative[0, 0] = -degree * (degree + 1) / 4.0
    derivative[degree, degree] = degree * (degree + 1) / 4.0
    stiff_ratio = (weights[:, None] * derivative**2).sum(0) / weights
    return (weights, derivative, stiff_ratio)


def clamped_gather(blocks):
    free_nodes = DEG * blocks - 1
    selector = np.zeros((free_nodes, blocks * (DEG + 1)), np.float32)
    for element in range(blocks):
        for node_idx in range(DEG + 1):
            target = DEG * element + node_idx - 1
            if 0 <= target < free_nodes:
                selector[target, element * (DEG + 1) + node_idx] = 1.0
    return selector


N1 = DEG + 1
SLOTS = 3
UNROLL = 6


def halves(value):
    high = value.astype(jnp.bfloat16)
    low = (value - high.astype(jnp.float32)).astype(jnp.bfloat16)
    return high, low


def np_halves(matrix):
    high = np.asarray(matrix, np.float32).astype(jnp.bfloat16)
    low = (np.asarray(matrix, np.float64) - high.astype(np.float64)).astype(jnp.bfloat16)
    return high, low


def apply_pairs(matrix, values, parity):
    half = N1 // 2
    even = [values[i] + values[DEG - i] for i in range(half)]
    odd = [values[i] - values[DEG - i] for i in range(half)]
    outs = [None] * N1
    for p in range(half):
        plus = None
        minus = None
        for i in range(half):
            by_even = float(np.float32((matrix[p, i] + matrix[p, DEG - i]) / 2))
            by_odd = float(np.float32((matrix[p, i] - matrix[p, DEG - i]) / 2))
            plus = by_even * even[i] if plus is None else plus + by_even * even[i]
            minus = by_odd * odd[i] if minus is None else minus + by_odd * odd[i]
        outs[p] = minus + plus
        outs[DEG - p] = plus - minus if parity > 0 else minus - plus
    return outs


def element_tables():
    weights, derivative, ratio = gll_tables(DEG)
    own = derivative.T * weights[None, :] / weights[:, None]
    second = own @ derivative
    return weights, derivative, ratio, own, second


class Loads:
    def __init__(self, places, staged, part_sem, whole_sem, put_sem):
        self.places = places
        self.staged = staged
        self.part_sem = part_sem
        self.whole_sem = whole_sem
        self.put_sem = put_sem

    def part(self, at, c):
        return pltpu.make_async_copy(
            self.places[at].at[c], self.staged[at].at[c], self.part_sem.at[at, c]
        )

    def whole(self, at):
        return pltpu.make_async_copy(self.places[at], self.staged[at], self.whole_sem.at[at])

    def put(self, at, out, c):
        return pltpu.make_async_copy(self.staged[at].at[c], out.at[c], self.put_sem.at[at, c])

    def start(self):
        self.whole(7).start()
        for c in range(3):
            self.part(0, c).start()
        for at in range(2, len(self.places)):
            if at != 7:
                self.whole(at).start()
        for c in range(3):
            self.part(1, c).start()

    def wait_part(self, at, c):
        self.part(at, c).wait()

    def wait_whole(self, at):
        self.whole(at).wait()


def smoother_kernel(
    steps,
    elems_x,
    elems_y,
    lame,
    upper,
    lower_ratio,
    loads,
    smoothed_out,
    residual_out,
    coef,
    field,
    resid,
    source,
    lam_w,
    mu_w,
    inverse,
    change,
    along_x,
    own_z,
    stress_x,
    part_x,
    arrived_x,
    arrived_y,
    scale_x,
    scale_y,
    rank_x,
    rank_y,
    rim,
    delta,
    narrow,
    wide,
    face_w,
    edge_lines,
    flat_a,
    flat_b,
    send_x,
    send_y,
    send_c,
    recv_x,
    recv_y,
    recv_c,
    send_sem,
    recv_sem,
):
    loads.start()
    (guess_in, source_in, material, weight_in, own_in, sum_in, spread_in, gather_in) = loads.staged[:8]
    (select_in, edge_in, own_mat, back_mat, second_mat, exact_mat, join_in) = loads.staged[8:]
    cols = elems_x * elems_y
    size_x = lax.axis_size("gx")
    size_y = lax.axis_size("gy")
    me_x = lax.axis_index("gx")
    me_y = lax.axis_index("gy")
    near_x = (lax.rem(me_x + size_x - 1, size_x), lax.rem(me_x + 1, size_x))
    near_y = (lax.rem(me_y + size_y - 1, size_y), lax.rem(me_y + 1, size_y))
    partners = [(near_x[0], me_y), (near_x[1], me_y), (me_x, near_y[0]), (me_x, near_y[1])]
    partners += [(near_x[a], near_y[b]) for a in range(2) for b in range(2)]

    barrier = pltpu.get_barrier_semaphore()
    for partner in partners:
        pl.semaphore_signal(
            barrier, inc=1, device_id=partner, device_id_type=pl.DeviceIdType.MESH
        )

    def copy_of(slot, d):
        if d < 2:
            src, dst = send_x.at[slot, d], recv_x.at[slot, 1 - d]
        elif d < 4:
            src, dst = send_y.at[slot, d - 2], recv_y.at[slot, 3 - d]
        else:
            src, dst = send_c.at[slot, d - 4], recv_c.at[slot, 7 - d]
        mirror = (1, 0, 3, 2, 7, 6, 5, 4)[d]
        return pltpu.make_async_remote_copy(
            src_ref=src,
            dst_ref=dst,
            send_sem=send_sem.at[slot, d],
            recv_sem=recv_sem.at[slot, mirror],
            device_id=partners[d],
            device_id_type=pl.DeviceIdType.MESH,
        )

    def start_all(slot, kinds):
        for d in kinds:
            copy_of(slot, d).start()

    def wait_for(slot, kinds):
        for d in kinds:
            copy_of(slot, d).wait()

    along_y = (2, 3)
    along_x_or_corner = (0, 1, 4, 5, 6, 7)
    every = range(8)

    rows = lax.broadcasted_iota(jnp.int32, (N1 * cols, 128), 0) % cols
    row_x = rows % elems_x
    inner_low_y = rows >= elems_x
    inner_high_y = rows < cols - elems_x
    inner_low_x = row_x >= 1
    inner_high_x = row_x < elems_x - 1
    last_x = elems_x - 1
    last_y = cols - elems_x
    flat = (N1 * cols, 128)
    full = (N1, cols, 128)

    def local_sum(ref, c):
        zero = jnp.zeros(flat, jnp.float32)
        low = ref[c, 0].reshape(flat)
        high = ref[c, DEG].reshape(flat)
        to_low = jnp.where(inner_low_x, pltpu.roll(high, 1, 0), zero)
        to_high = jnp.where(inner_high_x, pltpu.roll(low, N1 * cols - 1, 0), zero)
        ref[c, 0] = (low + to_low).reshape(full)
        ref[c, DEG] = (high + to_high).reshape(full)
        low = ref[c, :, 0].reshape(flat)
        high = ref[c, :, DEG].reshape(flat)
        to_low = jnp.where(inner_low_y, pltpu.roll(high, elems_x, 0), zero)
        to_high = jnp.where(inner_high_y, pltpu.roll(low, N1 * cols - elems_x, 0), zero)
        ref[c, :, 0] = (low + to_low).reshape(full)
        ref[c, :, DEG] = (high + to_high).reshape(full)

    def fill_y(ref, slot, c):
        send_y[slot, 0, c] = ref[c, :, 0, 0:elems_x, :]
        send_y[slot, 1, c] = ref[c, :, DEG, last_y:cols, :]

    def fill(ref, slot, c):
        fill_y(ref, slot, c)
        for b in range(elems_y):
            at = b * elems_x
            send_x[slot, 0, c, :, b : b + 1, :] = ref[c, 0, :, at : at + 1, :]
            at = b * elems_x + last_x
            send_x[slot, 1, c, :, b : b + 1, :] = ref[c, DEG, :, at : at + 1, :]
        for a in range(2):
            for b in range(2):
                at = a * last_x + b * last_y
                send_c[slot, 2 * a + b, c] = ref[c, a * DEG, b * DEG, at : at + 1, :]

    def collect(ref, slot, c):
        ref[c, :, 0, 0:elems_x, :] += recv_y[slot, 0, c]
        ref[c, :, DEG, last_y:cols, :] += recv_y[slot, 1, c]
        for b in range(elems_y):
            at = b * elems_x
            ref[c, 0, :, at : at + 1, :] += recv_x[slot, 0, c, :, b : b + 1, :]
            at = b * elems_x + last_x
            ref[c, DEG, :, at : at + 1, :] += recv_x[slot, 1, c, :, b : b + 1, :]
        for a in range(2):
            for b in range(2):
                at = a * last_x + b * last_y
                ref[c, a * DEG, b * DEG, at : at + 1, :] += recv_c[slot, 2 * a + b, c]

    nodes_x = DEG * elems_x
    nodes_y = DEG * elems_y
    nodes_z = guess_in.shape[2] // nodes_y
    pad_x = flat_a.shape[1]
    zeros_big = jnp.zeros((N1, cols, 128), jnp.float32)

    @pl.loop(0, nodes_y)
    def _(y):
        flat_a[y] = jnp.zeros((pad_x, 128), jnp.float32)
        flat_b[y] = jnp.zeros((pad_x, 128), jnp.float32)

    def through(src, dst, matrix):
        @pl.loop(0, elems_y, unroll=elems_y)
        def _(b):
            pick = pl.ds(b * DEG, DEG)
            parts = halves(src[pick].reshape(DEG * pad_x, 128))
            dst[pick] = jnp.dot(
                jnp.concatenate(parts, axis=1), matrix[...], preferred_element_type=jnp.float32
            ).reshape(DEG, pad_x, 128)

    def enter(flat_in, ref, c):
        lines = flat_in[c]
        for y in range(nodes_y):
            flat_a[y, 0:nodes_x, 0:nodes_z] = lines[:, y * nodes_z : (y + 1) * nodes_z]
        through(flat_a, flat_b, gather_in)
        ref[c, DEG] = zeros_big
        ref[c, :, DEG] = zeros_big
        for b in range(elems_y):
            for j in range(DEG):
                for i in range(DEG):
                    ref[c, i, j, b * elems_x : (b + 1) * elems_x, :] = flat_b[
                        b * DEG + j, pl.ds(i, elems_x, stride=DEG), :
                    ]

    def leave(ref, flat_out, c):
        for b in range(elems_y):
            for j in range(DEG):
                for i in range(DEG):
                    flat_b[b * DEG + j, pl.ds(i, elems_x, stride=DEG), :] = ref[
                        c, i, j, b * elems_x : (b + 1) * elems_x, :
                    ]
        through(flat_b, flat_a, select_in)
        lines = [flat_a[y, 0:nodes_x, 0:nodes_z] for y in range(nodes_y)]
        flat_out[c] = jnp.concatenate(lines, axis=1)

    loads.wait_whole(7)

    @pl.loop(0, 3)
    def _(c):
        loads.wait_part(0, c)
        enter(guess_in, field, c)
        local_sum(field, c)


    for at in range(2, len(loads.staged)):
        if at != 7:
            loads.wait_whole(at)
    upper_edge = jnp.full((1, 128), upper[0], jnp.float32)
    lower_edge = lower_ratio[0] * upper_edge
    center = (upper_edge + lower_edge) / 2.0
    radius = (upper_edge - lower_edge) / 2.0
    sigma_ratio = center / radius
    none_row = jnp.zeros((1, 128), jnp.float32)
    one_row = jnp.ones((1, 128), jnp.float32)
    coef[0, 0] = none_row
    coef[1, 0] = none_row
    coef[2, 0] = one_row
    for sweep in range(SWEEPS):
        first = sweep * CHEB + 1
        coef[0, first] = none_row
        coef[1, first] = 1.0 / center
        coef[2, first] = none_row
        factor = 1.0 / sigma_ratio
        for later in range(1, CHEB):
            factor_next = 1.0 / (2.0 * sigma_ratio - factor)
            coef[0, first + later] = factor_next * factor
            coef[1, first + later] = 2.0 * factor_next / radius
            coef[2, first + later] = none_row
            factor = factor_next

    kinds = jnp.concatenate([material[:, b, :] for b in range(elems_y)], axis=0)
    tables = []
    for row in range(2):
        picked = jnp.zeros(kinds.shape, jnp.float32)
        for kind in range(lame.shape[1]):
            picked = jnp.where(kinds == kind, lame[row, kind], picked)
        tables.append(
            jnp.dot(picked, spread_in[...], precision=highest, preferred_element_type=jnp.float32)
        )
    lam_all, mu_all = tables

    @pl.loop(0, N1)
    def _(i):
        for j in range(N1):
            lam_w[i, j] = lam_all * weight_in[i, j]
            mu_w[i, j] = mu_all * weight_in[i, j]

    @pl.loop(0, 3 * N1, unroll=N1)
    def _(at):
        c = at // N1
        i = at % N1
        pieces = []
        for j in range(N1):
            own = own_in[c, i, j]
            pieces.append(lam_w[i, j] * own + mu_w[i, j] * (sum_in[i, j] + own))
        high, low = halves(jnp.concatenate(pieces, axis=0))
        summed = jnp.dot(
            jnp.concatenate([high, low], axis=1), join_in[...], preferred_element_type=jnp.float32
        )
        inverse[c, i] = summed.reshape(N1, cols, 128)

    for c in range(3):
        local_sum(inverse, c)

    weights, derivative, _, own, second = element_tables()
    edge = float(np.float32(1.0 / weights[0]))
    groups = [slice(8 * h, 8 * h + 8) for h in range(cols // 8)]

    def product(parts, matrix):
        both = jnp.dot(
            jnp.concatenate(parts, axis=1), matrix[...], preferred_element_type=jnp.float32
        )
        return (both[:, :128] + both[:, 128:]).reshape(full)

    def forward(c, j, values):
        if c == 2:
            own_z[:, j] = product(halves(values.reshape(flat)), own_mat)
        for rows in groups:
            lines = [values[i, rows] for i in range(N1)]
            outs = apply_pairs(own, lines, -1) if c == 0 else apply_pairs(second, lines, 1)
            for i in range(N1):
                along_x[c, i, j, rows] = outs[i]

    def advance(c, step):
        alpha = coef[0, step]
        beta = coef[1, step]

        @pl.loop(0, N1, unroll=N1)
        def _(j):
            new = alpha * change[c, :, j] + beta * (inverse[c, :, j] * resid[c, :, j])
            change[c, :, j] = new
            new = field[c, :, j] + new
            field[c, :, j] = new
            forward(c, j, new)

    def sheet(i, edge_x):
        lines_y = []
        lines_v = []
        lines_z = []
        lines_t = []
        edge_z = edge_in[...]
        for rows in groups:
            u_x = [field[0, i, j, rows] for j in range(N1)]
            u_y = [field[1, i, j, rows] for j in range(N1)]
            u_z = [field[2, i, j, rows] for j in range(N1)]
            g_y = apply_pairs(own, u_y, -1)
            second_x = apply_pairs(second, u_x, 1)
            second_z = apply_pairs(second, u_z, 1)
            extra_y = []
            t_y = []
            group_v = []
            group_z = []
            group_t = []
            for j in range(N1):
                lam = lam_w[i, j, rows]
                mu = mu_w[i, j, rows]
                g_x = along_x[0, i, j, rows]
                g_z = own_z[i, j, rows]
                g_xy = g_x + g_y[j]
                e_z = edge_z * u_z[j]
                away_z = g_z - e_z
                shrink = g_xy + away_z
                own_x = g_x
                own_y = g_y[j]
                left = second_x[j]
                right = along_x[1, i, j, rows]
                if edge_x is not None:
                    e_x = edge_x * u_x[j]
                    shrink = shrink - e_x
                    own_x = g_x - (e_x + e_x)
                    left = left + edge_x * (g_y[j] + g_z)
                if j in (0, DEG):
                    edge_y = -edge if j == 0 else edge
                    e_y = edge_y * u_y[j]
                    shrink = shrink - e_y
                    own_y = g_y[j] - (e_y + e_y)
                    right = right + edge_y * (g_x + g_z)
                base = lam * shrink + mu * (g_xy + g_z)
                stress_x[i, j, rows] = base + mu * own_x
                part_x[i, j, rows] = mu * left
                t_y.append(base + mu * own_y)
                extra_y.append(mu * right)
                group_v.append(mu * u_y[j])
                group_t.append(base + mu * (away_z - e_z))
                group_z.append(mu * ((along_x[2, i, j, rows] + second_z[j]) + edge_z * g_xy))
            back_y = apply_pairs(-derivative.T, t_y, -1)
            lines_y.append([back_y[j] + extra_y[j] for j in range(N1)])
            lines_v.append(group_v)
            lines_z.append(group_z)
            lines_t.append(group_t)

        def stacked(lines):
            return jnp.concatenate([lines[h][j] for j in range(N1) for h in range(len(groups))], axis=0)

        parts = halves(stacked(lines_y)) + halves(stacked(lines_v))
        resid[1, i] = source[1, i] - product(parts, second_mat)
        parts = halves(stacked(lines_z)) + halves(stacked(lines_t))
        resid[2, i] = source[2, i] - product(parts, back_mat)

    def closing(j):
        lines_x = []
        lines_v = []
        for rows in groups:
            back_x = apply_pairs(-derivative.T, [stress_x[i, j, rows] for i in range(N1)], -1)
            lines_x.append([part_x[i, j, rows] + back_x[i] for i in range(N1)])
            lines_v.append([mu_w[i, j, rows] * field[0, i, j, rows] for i in range(N1)])

        def stacked(lines):
            return jnp.concatenate([lines[h][i] for i in range(N1) for h in range(len(groups))], axis=0)

        parts = halves(stacked(lines_x)) + halves(stacked(lines_v))
        resid[0, :, j] = source[0, :, j] - product(parts, second_mat)

    def volume(step, slot):
        for c in (1, 2, 0):
            advance(c, step)

        @pl.loop(1, DEG, unroll=UNROLL)
        def _(i):
            sheet(i, None)

        for side in range(2):
            sheet(side * DEG, edge if side else -edge)

        wait_for(slot, along_y)

        @pl.loop(0, N1, unroll=N1)
        def _(j):
            closing(j)

    arrived = (arrived_x, arrived_y)
    scale = (scale_x, scale_y)
    per_side = (elems_y, elems_x)
    ring = 2 * elems_x
    windows = (slice(0, ring), slice(cols - ring, cols))
    row_id = lax.broadcasted_iota(jnp.int32, (cols, 128), 0)
    ring_id = [lax.broadcasted_iota(jnp.int32, (2 * size, 128), 0) for size in per_side]
    low_side = [ring_id[axis] < per_side[axis] for axis in range(2)]
    place_t = [ring_id[axis] % per_side[axis] for axis in range(2)]
    lines_low = pl.ds(0, elems_y, stride=elems_x)
    lines_high = pl.ds(last_x, elems_y, stride=elems_x)

    def by_side(axis, low, high):
        return jnp.where(low_side[axis], low, high)

    def rank_tables():
        for axis in range(2):
            for p in range(N1):
                rows = []
                for f in (0, DEG):
                    others = [k for k in range(N1) if k != f]
                    chain = sum(derivative[k, p] * weights[k] * own[k, f] for k in others)
                    away = float(p != f)
                    heavy = away * weights[p]
                    rows.append((away * derivative[f, p], -away * chain, heavy * second[p, f], heavy * own[p, f]))
                for kind in range(4):
                    low, high = (float(np.float32(row[kind])) for row in rows)
                    if axis == 0:
                        col = row_id % elems_x
                        rank_x[kind, p] = jnp.where(col == 0, low, jnp.where(col == last_x, high, 0.0))
                    else:
                        rank_y[0, kind, p] = by_side(1, low, 0.0)
                        rank_y[1, kind, p] = by_side(1, 0.0, high)

    def gather_x(ref, c, low, high, dst, at):
        half = per_side[0]
        for t in range(N1):
            dst[at, t, 0:half, :] = ref[c, low, t, lines_low, :]
            dst[at, t, half : 2 * half, :] = ref[c, high, t, lines_high, :]

    def face_y(ref, c, t):
        return jnp.where(low_side[1], ref[c, t, 0, windows[0]], ref[c, t, DEG, windows[1]])

    def add_y(ref, c, t, value):
        ref[c, t, 0, windows[0]] = ref[c, t, 0, windows[0]] + by_side(1, value, 0.0)
        ref[c, t, DEG, windows[1]] = ref[c, t, DEG, windows[1]] + by_side(1, 0.0, value)

    def add_x(ref, c, t):
        half = per_side[0]
        ref[c, 0, t, lines_low, :] = ref[c, 0, t, lines_low, :] + delta[c, t, 0:half, :]
        ref[c, DEG, t, lines_high, :] = ref[c, DEG, t, lines_high, :] + delta[c, t, half : 2 * half, :]

    def face_weights():
        half = per_side[0]
        for kind, ref in enumerate((lam_w, mu_w)):
            for t in range(N1):
                face_w[0, kind, t, 0:half, :] = ref[0, t, lines_low, :]
                face_w[0, kind, t, half : 2 * half, :] = ref[0, t, lines_high, :]
                face_w[1, kind, t] = jnp.where(low_side[1], ref[0, t, windows[0]], ref[0, t, windows[1]])

    def face_scales():
        for c in range(3):
            gather_x(inverse, c, 0, DEG, scale_x, c)
            for t in range(N1):
                scale_y[c, t] = face_y(inverse, c, t)

    def arrive_y(slot):
        for c in range(3):
            arrived_y[c, :, 0:elems_x, :] = recv_y[slot, 0, c]
            arrived_y[c, :, elems_x:ring, :] = recv_y[slot, 1, c]

    def arrive_x(slot):
        half = per_side[0]
        for c in range(3):
            arrived_x[c, :, 0:half, :] = recv_x[slot, 0, c]
            arrived_x[c, :, half : 2 * half, :] = recv_x[slot, 1, c]
            for a in range(2):
                for b in range(2):
                    at = a * half + b * (half - 1)
                    arrived_x[c, b * DEG, at : at + 1, :] += (
                        recv_c[slot, 2 * a + b, c] + recv_y[slot, b, c, a * DEG, a * last_x : a * last_x + 1, :]
                    )

    def send_rim(slot):
        half = per_side[0]
        for c in range(3):
            low = rim[c, 0]
            high = rim[c, DEG]
            rim[c, 0] = low + jnp.where(place_t[0] >= 1, pltpu.roll(high, 1, 0), 0.0)
            rim[c, DEG] = high + jnp.where(place_t[0] < half - 1, pltpu.roll(low, 2 * half - 1, 0), 0.0)
            send_x[slot, 0, c] = rim[c, :, 0:half, :]
            send_x[slot, 1, c] = rim[c, :, half : 2 * half, :]
            for a in range(2):
                for b in range(2):
                    at = a * half + b * (half - 1)
                    send_c[slot, 2 * a + b, c] = rim[c, b * DEG, at : at + 1, :]
        start_all(slot, along_x_or_corner)

    def correct(axis, step, slot):
        normal, side = axis, 1 - axis
        beta = coef[1, step]
        plain = coef[2, step]
        edge_z = edge_in[...]
        edge_n = by_side(axis, -edge, edge)
        own_f = by_side(axis, float(np.float32(own[0, 0])), float(np.float32(own[DEG, DEG])))
        second_f = float(np.float32(second[0, 0]))
        per_w = float(np.float32(1.0 / weights[0]))
        chain_f = [sum(derivative[k, f] * weights[k] * own[k, f] for k in range(N1) if k != f) for f in (0, DEG)]
        first_f = by_side(axis, float(np.float32(derivative[0, 0])), float(np.float32(derivative[DEG, DEG])))
        then_f = by_side(axis, *(float(np.float32(-value)) for value in chain_f))
        size = 2 * per_side[axis]
        half = per_side[0]
        d = [[None] * N1 for _ in range(3)]
        for c in range(3):
            for t in range(N1):
                value = (plain + beta * scale[axis][c, t]) * arrived[axis][c, t]
                if axis == 1 and t in (0, DEG):
                    value = jnp.where(place_t[1] == (0 if t == 0 else last_x), 0.0, value)
                d[c][t] = value
        d_n, d_t, d_z = d[normal], d[side], d[2]

        def stack(lines):
            return jnp.concatenate(lines, axis=0)

        def joint(parts, matrix, count):
            both = jnp.dot(
                jnp.concatenate(parts, axis=1), matrix[...], preferred_element_type=jnp.float32
            )
            return (both[:, :128] + both[:, 128:]).reshape(count, N1, size, 128)

        g_z = joint(halves(stack(d_z)), own_mat, 1)[0]
        g_t = apply_pairs(own, d_t, -1)
        second_n = apply_pairs(second, d_n, 1)
        second_z = apply_pairs(second, d_z, 1)
        t_n, t_t, t_z, left, v_n, v_t, extra, f_z = [[] for _ in range(8)]
        stiff, mixed, mixed_t, mixed_z, one_t, one_z = [[] for _ in range(6)]
        for t in range(N1):
            lam = face_w[axis, 0, t]
            mu = face_w[axis, 1, t]
            g_n = own_f * d_n[t]
            g_nt = g_n + g_t[t]
            e_n = edge_n * d_n[t]
            e_z = edge_z * d_z[t]
            away_z = g_z[t] - e_z
            shrink = (g_nt + away_z) - e_n
            own_t = g_t[t]
            right = second_f * d_t[t]
            mu_d = mu * d_n[t]
            mu_in = per_w * mu_d
            mixed.append(per_w * (lam * d_n[t]) + mu_in)
            stiff.append(mixed[t] + mu_in)
            if t in (0, DEG):
                edge_t = -edge if t == 0 else edge
                e_t = edge_t * d_t[t]
                shrink = shrink - e_t
                own_t = own_t - (e_t + e_t)
                right = right + edge_t * (g_n + g_z[t])
                mixed_t.append(edge_t * mu_in)
            else:
                mixed_t.append(None)
            base = lam * shrink + mu * (g_nt + g_z[t])
            t_n.append(base + mu * (g_n - (e_n + e_n)))
            t_t.append(base + mu * own_t)
            t_z.append(base + mu * (away_z - e_z))
            left.append(mu * (second_n[t] + edge_n * (g_t[t] + g_z[t])))
            v_n.append(mu_d)
            v_t.append(mu * d_t[t])
            extra.append(mu * right)
            f_z.append(mu * ((second_f * d_z[t] + second_z[t]) + edge_z * g_nt))
            mixed_z.append(edge_z * mu_in)
            one_t.append(per_w * v_t[t])
            one_z.append(per_w * (mu * d_z[t]))
        back_t = apply_pairs(-derivative.T, t_t, -1)
        back_m = apply_pairs(-derivative.T, mixed, -1)
        f_t = [back_t[t] + extra[t] for t in range(N1)]
        two_t = [back_m[t] if mixed_t[t] is None else back_m[t] + mixed_t[t] for t in range(N1)]
        parts = halves(stack(left + f_t)) + halves(stack(v_n + v_t))
        faces = joint(parts, second_mat, 2)
        parts = halves(stack(f_z)) + halves(stack(t_z))
        face_z = joint(parts, back_mat, 1)[0]

        def joined(lines, count):
            return jnp.dot(
                jnp.concatenate(halves(stack(lines)), axis=1),
                exact_mat[...],
                preferred_element_type=jnp.float32,
            ).reshape(count, N1, size, 128)

        along_n = joined(t_n + stiff, 2)
        away = joined(one_t + two_t + one_z, 3)
        parts = halves(stack(mixed_z)) + halves(stack(mixed))
        upright = joint(parts, back_mat, 1)[0]
        at_face = {normal: faces[0], side: faces[1], 2: face_z}
        if axis == 0:
            for c in range(3):
                gather_x(resid, c, 0, DEG, rim, c)
        for c in range(3):
            for t in range(N1):
                value = at_face[c][t]
                if c == normal:
                    value = value + (then_f * along_n[1, t] - first_f * along_n[0, t])
                if axis == 0:
                    left_over = rim[c, t] - value
                    rim[c, t] = left_over
                    delta[c, t] = left_over
                else:
                    add_y(resid, c, t, -value)
        if axis == 0:
            for c in range(3):
                for t in range(N1):
                    resid[c, 0, t, lines_low, :] = delta[c, t, 0:half, :]
                    resid[c, DEG, t, lines_high, :] = delta[c, t, half : 2 * half, :]
            send_rim(slot)
        pairs = {normal: (0, -along_n[0], along_n[1]), side: (2, away[0], away[1]), 2: (2, away[2], upright)}
        for c in range(3):
            for t in range(N1):
                if axis == 0:
                    delta[c, t] = d[c][t]
                    add_x(field, c, t)
                    add_x(change, c, t)
                else:
                    add_y(field, c, t, d[c][t])
                    add_y(change, c, t, d[c][t])
        for t in range(N1):
            for c in range(3):
                kind, first, then = pairs[c]
                if axis == 0:
                    for k, value in enumerate((first[t], then[t])):
                        narrow[2 * c + k, t] = value
                        wide[2 * c + k, t, lines_low, :] = narrow[2 * c + k, t, 0:half, :]
                        wide[2 * c + k, t, lines_high, :] = narrow[2 * c + k, t, half : 2 * half, :]
                    first_t, then_t = wide[2 * c, t], wide[2 * c + 1, t]
                    for p in range(N1):
                        change_by = rank_x[kind, p] * first_t + rank_x[kind + 1, p] * then_t
                        resid[c, p, t] = resid[c, p, t] - change_by
                else:
                    for p in range(N1):
                        for w, rows in enumerate(windows):
                            change_by = rank_y[w, kind, p] * first[t] + rank_y[w, kind + 1, p] * then[t]
                            resid[c, t, p, rows] = resid[c, t, p, rows] - change_by

    @pl.loop(0, 3)
    def _(c):
        loads.wait_part(1, c)
        enter(source_in, source, c)

    rank_tables()
    face_weights()
    for ref in (scale_x, scale_y, wide):
        ref[...] = jnp.zeros(ref.shape, jnp.float32)

    for c in range(3):

        @pl.loop(0, N1)
        def _(i):
            change[c, i] = zeros_big
            resid[c, i] = zeros_big

    for c in range(3):
        fill(field, 0, c)
        fill(inverse, 2, c)

    pl.semaphore_wait(barrier, len(partners))

    start_all(0, every)
    start_all(2, every)

    @pl.loop(0, steps + 1)
    def _(step):
        slot = step % 2
        volume(step, slot)
        arrive_y(slot)
        correct(1, step, 1 - slot)
        wait_for(slot, along_x_or_corner)
        arrive_x(slot)
        correct(0, step, 1 - slot)

        @pl.loop(0, 3)
        def _(c):
            local_sum(resid, c)
            fill_y(resid, 1 - slot, c)

        start_all(1 - slot, along_y)

        @pl.when(step == 0)
        def _():
            wait_for(2, every)

            @pl.loop(0, 3)
            def _(c):
                collect(inverse, 2, c)

                @pl.loop(0, N1)
                def _(i):
                    inverse[c, i] = 1.0 / inverse[c, i]

            face_scales()

    @pl.loop(0, 3)
    def _(c):
        leave(field, guess_in, c)
        loads.put(0, smoothed_out, c).start()

    @pl.loop(0, 3)
    def _(c):
        leave(resid, source_in, c)

    edge_lines[...] = jnp.zeros(edge_lines.shape, jnp.float32)
    slot = (steps + 1) % 2
    wait_for(slot, every)
    arrive_y(slot)
    arrive_x(slot)
    for c in range(3):
        for t in range(DEG):
            edge_lines[c, 0, pl.ds(t, elems_y, stride=DEG), :] = arrived_x[c, t, 0:elems_y, :]
            edge_lines[c, 1, pl.ds(t, elems_x, stride=DEG), :] = arrived_y[c, t, 0:elems_x, :]
        edge_lines[c, 1, 0:1, :] = jnp.zeros((1, 128), jnp.float32)
    depth = edge_lines.shape[2]
    parts = halves(edge_lines[...].reshape(6 * depth, 128))
    found = jnp.dot(
        jnp.concatenate(parts, axis=1), select_in[...], preferred_element_type=jnp.float32
    ).reshape(3, 2, depth, 128)
    for c in range(3):
        pieces = [found[c, 0, y : y + 1, 0:nodes_z] for y in range(nodes_y)]
        source_in[c, 0:1, :] = source_in[c, 0:1, :] + jnp.concatenate(pieces, axis=1)
        source_in[c, :, 0:nodes_z] = source_in[c, :, 0:nodes_z] + found[c, 1, 0:nodes_x, 0:nodes_z]
        loads.put(1, residual_out, c).start()

    @pl.loop(0, 3)
    def _(c):
        loads.put(0, smoothed_out, c).wait()
        loads.put(1, residual_out, c).wait()


def z_join(blocks, clamped):
    nodes = DEG * blocks + 1
    gather = np.zeros((nodes, blocks * N1))
    for element in range(blocks):
        for k in range(N1):
            gather[DEG * element + k, element * N1 + k] = 1.0
    if clamped:
        gather[0] = 0.0
        gather[nodes - 1] = 0.0
    return gather.T @ gather


def local(right_side, guess, material, lame, upper, lower_ratio):
    elems_x, elems_y, elems_z = material.shape
    cols = elems_x * elems_y
    lanes = N1 * elems_z
    nodes_z = DEG * elems_z - 1
    weights_np, derivative_np, ratio_np, own_np_1, second_np = element_tables()
    eye_z = np.eye(elems_z)
    join_np = z_join(elems_z, True)
    joined = join_np.astype(jnp.bfloat16)

    def exact_pair(matrix):
        high, low = np_halves(matrix)
        none = np.zeros_like(high)
        return [[high, low], [high, none]]

    exact_join = [[joined, np.zeros_like(joined)]] * 2
    own_mat = jnp.asarray(np.block(exact_pair(np.kron(eye_z, own_np_1.T))))
    back_np = np.kron(eye_z, derivative_np) @ join_np
    back_mat = jnp.asarray(np.block(exact_join + exact_pair(-back_np)))
    scaled_np = np.kron(eye_z, second_np) @ join_np
    second_mat = jnp.asarray(np.block(exact_join + exact_pair(scaled_np)))
    exact_mat = jnp.asarray(np.concatenate([joined, joined], axis=0))
    edge_np = np.zeros((1, lanes))
    edge_np[0, 0::N1] = -1.0 / weights_np[0]
    edge_np[0, DEG::N1] = 1.0 / weights_np[DEG]
    edge_in = jnp.asarray(edge_np, jnp.float32)
    all_join = z_join(elems_z, False).astype(jnp.bfloat16)
    join_in = jnp.asarray(np.concatenate([all_join, all_join], axis=0))

    weights_z = np.tile(weights_np, elems_z)
    ratio_z = np.tile(ratio_np, elems_z)
    weight_np = weights_np[:, None, None] * weights_np[None, :, None] * weights_z
    shape_w = (N1, N1, lanes)
    own_x = np.broadcast_to(ratio_np[:, None, None], shape_w)
    own_y = np.broadcast_to(ratio_np[None, :, None], shape_w)
    own_z = np.broadcast_to(ratio_z, shape_w)
    own_np = np.stack([own_x, own_y, own_z])
    weight_in = jnp.asarray(weight_np[:, :, None], jnp.float32)
    own_in = jnp.asarray(own_np[:, :, :, None], jnp.float32)
    sum_in = jnp.asarray((own_x + own_y + own_z)[:, :, None], jnp.float32)

    gather_np = clamped_gather(elems_z)
    nodes_z = gather_np.shape[0]
    owned_np = gather_np.copy()
    owned_np[:, DEG::N1] = 0.0
    enter_np = np.zeros((lanes, lanes))
    enter_np[:nodes_z] = gather_np
    leave_np = np.zeros((lanes, lanes))
    leave_np[:, :nodes_z] = owned_np.T
    gather_in = jnp.asarray(np.concatenate([enter_np, enter_np], axis=0).astype(jnp.bfloat16))
    select_in = jnp.asarray(np.concatenate([leave_np, leave_np], axis=0).astype(jnp.bfloat16))
    spread_in = jnp.asarray(np.kron(eye_z, np.ones((1, N1))), dtype=jnp.float32)

    pad_x = -(-DEG * elems_x // 8) * 8
    whole = (3, N1, N1, cols, lanes)
    smem = pl.BlockSpec(memory_space=pltpu.SMEM)
    big = pltpu.VMEM(whole, jnp.float32)
    small = pltpu.VMEM((N1, N1, cols, lanes), jnp.float32)
    ring = 2 * elems_x
    face_a = pltpu.VMEM((3, N1, 2 * elems_y, lanes), jnp.float32)
    face_b = pltpu.VMEM((3, N1, ring, lanes), jnp.float32)
    edge_size = -(-DEG * max(elems_x, elems_y) // 8) * 8
    lines = pltpu.VMEM((DEG * elems_y, pad_x, lanes), jnp.float32)
    face_x = pltpu.VMEM((SLOTS, 2, 3, N1, elems_y, lanes), jnp.float32)
    face_y = pltpu.VMEM((SLOTS, 2, 3, N1, elems_x, lanes), jnp.float32)
    corner = pltpu.VMEM((SLOTS, 4, 3, 1, lanes), jnp.float32)
    shape = jax.ShapeDtypeStruct(guess.shape, jnp.float32)

    operands = [
        guess,
        right_side,
        material,
        weight_in,
        own_in,
        sum_in,
        spread_in,
        gather_in,
        select_in,
        edge_in,
        own_mat,
        back_mat,
        second_mat,
        exact_mat,
        join_in,
    ]
    number = len(operands)

    def kernel(*refs):
        scalars, places, outs = refs[:3], refs[3 : 3 + number], refs[3 + number : 5 + number]
        staged, rest = refs[5 + number : 5 + 2 * number], refs[5 + 2 * number :]
        loads = Loads(places, staged, *rest[:3])
        smoother_kernel(SWEEPS * CHEB, elems_x, elems_y, *scalars, loads, *outs, *rest[3:])

    away = pl.BlockSpec(memory_space=pl.ANY)
    return pl.pallas_call(
        kernel,
        out_shape=(shape, shape),
        in_specs=[smem] * 3 + [away] * number,
        out_specs=(away, away),
        scratch_shapes=[pltpu.VMEM(operand.shape, operand.dtype) for operand in operands]
        + [pltpu.SemaphoreType.DMA((2, 3)), pltpu.SemaphoreType.DMA((number,)), pltpu.SemaphoreType.DMA((2, 3))]
        + [pltpu.VMEM((3, SWEEPS * CHEB + 1, 1, lanes), jnp.float32)]
        + [big] * 3
        + [small] * 2
        + [big] * 3
        + [small] * 3
        + [face_a, face_b] * 2
        + [pltpu.VMEM((4, N1, cols, lanes), jnp.float32)]
        + [pltpu.VMEM((2, 4, N1, ring, lanes), jnp.float32)]
        + [face_a] * 2
        + [pltpu.VMEM((6, N1, 2 * elems_y, lanes), jnp.float32)]
        + [pltpu.VMEM((6, N1, cols, lanes), jnp.float32)]
        + [pltpu.VMEM((2, 2, N1, ring, lanes), jnp.float32)]
        + [pltpu.VMEM((3, 2, edge_size, lanes), jnp.float32)]
        + [lines] * 2
        + [face_x, face_y, corner] * 2
        + [pltpu.SemaphoreType.DMA((SLOTS, 8))] * 2,
        compiler_params=pltpu.CompilerParams(collective_id=0, has_side_effects=True),
    )(lame, upper, lower_ratio, *operands)


def solution(mesh):
    placed = (P(None, "gx", "gy"), P(None, "gx", "gy"), P("gx", "gy", None), P(), P(), P())
    return jax.shard_map(
        local,
        mesh=mesh,
        in_specs=placed,
        out_specs=(P(None, "gx", "gy"), P(None, "gx", "gy")),
        check_vma=False,
    )
```

```python
import jax
import jax.numpy as jnp
import numpy as np
from jax import lax
from jax.experimental import pallas as pl
from jax.experimental.pallas import tpu as pltpu
from jax.sharding import PartitionSpec as P

DEG = 7
SWEEPS = 2
CHEB = 3


highest = lax.Precision.HIGHEST


def legendre_pair(points, degree):
    prev_poly = points * 0.0 + 1.0
    this_poly = points * 1.0
    for order in range(2, degree + 1):
        next_poly = ((2 * order - 1) * points * this_poly - (order - 1) * prev_poly) / order
        prev_poly = this_poly
        this_poly = next_poly
    return (this_poly, prev_poly)


def gll_tables(degree):
    count = degree + 1
    points = -np.cos(np.pi * np.arange(count) / degree)
    for newton_step in range(60):
        this_poly, prev_poly = legendre_pair(points, degree)
        points = points - (points * this_poly - prev_poly) / (count * this_poly)
    values, unused_poly = legendre_pair(points, degree)
    weights = 2.0 / (degree * (degree + 1) * values**2)
    identity_np = np.eye(count)
    spacing = points[:, None] - points[None, :] + identity_np
    derivative = values[:, None] / (values[None, :] * spacing) * (1.0 - identity_np)
    derivative[0, 0] = -degree * (degree + 1) / 4.0
    derivative[degree, degree] = degree * (degree + 1) / 4.0
    stiff_ratio = (weights[:, None] * derivative**2).sum(0) / weights
    return (weights, derivative, stiff_ratio)


def clamped_gather(blocks):
    free_nodes = DEG * blocks - 1
    selector = np.zeros((free_nodes, blocks * (DEG + 1)), np.float32)
    for element in range(blocks):
        for node_idx in range(DEG + 1):
            target = DEG * element + node_idx - 1
            if 0 <= target < free_nodes:
                selector[target, element * (DEG + 1) + node_idx] = 1.0
    return selector


N1 = DEG + 1
SLOTS = 3
UNROLL = 6
VMEM_BYTES = 36 * 1024 * 1024


def halves(value):
    high = value.astype(jnp.bfloat16)
    low = (value - high.astype(jnp.float32)).astype(jnp.bfloat16)
    return high, low


def np_halves(matrix):
    high = np.asarray(matrix, np.float32).astype(jnp.bfloat16)
    low = (np.asarray(matrix, np.float64) - high.astype(np.float64)).astype(jnp.bfloat16)
    return high, low


def apply_pairs(matrix, values, parity):
    half = N1 // 2
    even = [values[i] + values[DEG - i] for i in range(half)]
    odd = [values[i] - values[DEG - i] for i in range(half)]
    outs = [None] * N1
    for p in range(half):
        plus = None
        minus = None
        for i in range(half):
            by_even = float(np.float32((matrix[p, i] + matrix[p, DEG - i]) / 2))
            by_odd = float(np.float32((matrix[p, i] - matrix[p, DEG - i]) / 2))
            plus = by_even * even[i] if plus is None else plus + by_even * even[i]
            minus = by_odd * odd[i] if minus is None else minus + by_odd * odd[i]
        outs[p] = minus + plus
        outs[DEG - p] = plus - minus if parity > 0 else minus - plus
    return outs


def element_tables():
    weights, derivative, ratio = gll_tables(DEG)
    own = derivative.T * weights[None, :] / weights[:, None]
    second = own @ derivative
    return weights, derivative, ratio, own, second


class Loads:
    def __init__(self, places, staged, part_sem, whole_sem):
        self.places = places
        self.staged = staged
        self.part_sem = part_sem
        self.whole_sem = whole_sem

    def part(self, at, c):
        return pltpu.make_async_copy(
            self.places[at].at[c], self.staged[at].at[c], self.part_sem.at[at, c]
        )

    def whole(self, at):
        return pltpu.make_async_copy(self.places[at], self.staged[at], self.whole_sem.at[at])

    def start(self):
        self.whole(7).start()
        for c in range(3):
            self.part(0, c).start()
        for at in range(2, len(self.places)):
            if at != 7:
                self.whole(at).start()
        for c in range(3):
            self.part(1, c).start()

    def wait_part(self, at, c):
        self.part(at, c).wait()

    def wait_whole(self, at):
        self.whole(at).wait()


def smoother_kernel(
    steps,
    elems_x,
    elems_y,
    lame,
    upper,
    lower_ratio,
    loads,
    smoothed_out,
    residual_out,
    patch_out,
    coef,
    field,
    resid,
    source,
    lam_w,
    mu_w,
    inverse,
    change,
    along_x,
    own_z,
    stress_x,
    part_x,
    arrived_x,
    arrived_y,
    scale_x,
    scale_y,
    rank_x,
    rank_y,
    rim,
    delta,
    narrow,
    wide,
    face_w,
    edge_lines,
    flat_a,
    flat_b,
    send_x,
    send_y,
    send_c,
    recv_x,
    recv_y,
    recv_c,
    send_sem,
    recv_sem,
):
    loads.start()
    (guess_in, source_in, material, weight_in, own_in, sum_in, spread_in, gather_in) = loads.staged[:8]
    (select_in, edge_in, own_mat, back_mat, second_mat, exact_mat, join_in) = loads.staged[8:]
    cols = elems_x * elems_y
    size_x = lax.axis_size("gx")
    size_y = lax.axis_size("gy")
    me_x = lax.axis_index("gx")
    me_y = lax.axis_index("gy")
    near_x = (lax.rem(me_x + size_x - 1, size_x), lax.rem(me_x + 1, size_x))
    near_y = (lax.rem(me_y + size_y - 1, size_y), lax.rem(me_y + 1, size_y))
    partners = [(near_x[0], me_y), (near_x[1], me_y), (me_x, near_y[0]), (me_x, near_y[1])]
    partners += [(near_x[a], near_y[b]) for a in range(2) for b in range(2)]

    barrier = pltpu.get_barrier_semaphore()
    for partner in partners:
        pl.semaphore_signal(
            barrier, inc=1, device_id=partner, device_id_type=pl.DeviceIdType.MESH
        )

    def copy_of(slot, d):
        if d < 2:
            src, dst = send_x.at[slot, d], recv_x.at[slot, 1 - d]
        elif d < 4:
            src, dst = send_y.at[slot, d - 2], recv_y.at[slot, 3 - d]
        else:
            src, dst = send_c.at[slot, d - 4], recv_c.at[slot, 7 - d]
        mirror = (1, 0, 3, 2, 7, 6, 5, 4)[d]
        return pltpu.make_async_remote_copy(
            src_ref=src,
            dst_ref=dst,
            send_sem=send_sem.at[slot, d],
            recv_sem=recv_sem.at[slot, mirror],
            device_id=partners[d],
            device_id_type=pl.DeviceIdType.MESH,
        )

    def start_all(slot, kinds):
        for d in kinds:
            copy_of(slot, d).start()

    def wait_for(slot, kinds):
        for d in kinds:
            copy_of(slot, d).wait()

    along_y = (2, 3)
    along_x_or_corner = (0, 1, 4, 5, 6, 7)
    every = range(8)

    rows = lax.broadcasted_iota(jnp.int32, (N1 * cols, 128), 0) % cols
    row_x = rows % elems_x
    inner_low_y = rows >= elems_x
    inner_high_y = rows < cols - elems_x
    inner_low_x = row_x >= 1
    inner_high_x = row_x < elems_x - 1
    last_x = elems_x - 1
    last_y = cols - elems_x
    flat = (N1 * cols, 128)
    full = (N1, cols, 128)

    def local_sum(ref, c):
        zero = jnp.zeros(flat, jnp.float32)
        low = ref[c, 0].reshape(flat)
        high = ref[c, DEG].reshape(flat)
        to_low = jnp.where(inner_low_x, pltpu.roll(high, 1, 0), zero)
        to_high = jnp.where(inner_high_x, pltpu.roll(low, N1 * cols - 1, 0), zero)
        ref[c, 0] = (low + to_low).reshape(full)
        ref[c, DEG] = (high + to_high).reshape(full)
        low = ref[c, :, 0].reshape(flat)
        high = ref[c, :, DEG].reshape(flat)
        to_low = jnp.where(inner_low_y, pltpu.roll(high, elems_x, 0), zero)
        to_high = jnp.where(inner_high_y, pltpu.roll(low, N1 * cols - elems_x, 0), zero)
        ref[c, :, 0] = (low + to_low).reshape(full)
        ref[c, :, DEG] = (high + to_high).reshape(full)

    def fill_y(ref, slot, c):
        send_y[slot, 0, c] = ref[c, :, 0, 0:elems_x, :]
        send_y[slot, 1, c] = ref[c, :, DEG, last_y:cols, :]

    def fill(ref, slot, c):
        fill_y(ref, slot, c)
        for b in range(elems_y):
            at = b * elems_x
            send_x[slot, 0, c, :, b : b + 1, :] = ref[c, 0, :, at : at + 1, :]
            at = b * elems_x + last_x
            send_x[slot, 1, c, :, b : b + 1, :] = ref[c, DEG, :, at : at + 1, :]
        for a in range(2):
            for b in range(2):
                at = a * last_x + b * last_y
                send_c[slot, 2 * a + b, c] = ref[c, a * DEG, b * DEG, at : at + 1, :]

    def collect(ref, slot, c):
        ref[c, :, 0, 0:elems_x, :] += recv_y[slot, 0, c]
        ref[c, :, DEG, last_y:cols, :] += recv_y[slot, 1, c]
        for b in range(elems_y):
            at = b * elems_x
            ref[c, 0, :, at : at + 1, :] += recv_x[slot, 0, c, :, b : b + 1, :]
            at = b * elems_x + last_x
            ref[c, DEG, :, at : at + 1, :] += recv_x[slot, 1, c, :, b : b + 1, :]
        for a in range(2):
            for b in range(2):
                at = a * last_x + b * last_y
                ref[c, a * DEG, b * DEG, at : at + 1, :] += recv_c[slot, 2 * a + b, c]

    nodes_x = DEG * elems_x
    nodes_y = DEG * elems_y
    nodes_z = guess_in.shape[2] // nodes_y
    pad_x = flat_a.shape[1]
    zeros_big = jnp.zeros((N1, cols, 128), jnp.float32)

    @pl.loop(0, nodes_y)
    def _(y):
        flat_a[y] = jnp.zeros((pad_x, 128), jnp.float32)
        flat_b[y] = jnp.zeros((pad_x, 128), jnp.float32)

    def through(src, dst, matrix):
        @pl.loop(0, elems_y, unroll=elems_y)
        def _(b):
            pick = pl.ds(b * DEG, DEG)
            parts = halves(src[pick].reshape(DEG * pad_x, 128))
            dst[pick] = jnp.dot(
                jnp.concatenate(parts, axis=1), matrix[...], preferred_element_type=jnp.float32
            ).reshape(DEG, pad_x, 128)

    def enter(flat_in, ref, c):
        lines = flat_in[c]
        for y in range(nodes_y):
            flat_a[y, 0:nodes_x, 0:nodes_z] = lines[:, y * nodes_z : (y + 1) * nodes_z]
        through(flat_a, flat_b, gather_in)
        ref[c, DEG] = zeros_big
        ref[c, :, DEG] = zeros_big
        for b in range(elems_y):
            for j in range(DEG):
                for i in range(DEG):
                    ref[c, i, j, b * elems_x : (b + 1) * elems_x, :] = flat_b[
                        b * DEG + j, pl.ds(i, elems_x, stride=DEG), :
                    ]

    def leave(ref, flat_out, c):
        for b in range(elems_y):
            for j in range(DEG):
                for i in range(DEG):
                    flat_b[b * DEG + j, pl.ds(i, elems_x, stride=DEG), :] = ref[
                        c, i, j, b * elems_x : (b + 1) * elems_x, :
                    ]
        through(flat_b, flat_a, select_in)
        lines = [flat_a[y, 0:nodes_x, 0:nodes_z] for y in range(nodes_y)]
        flat_out[c] = jnp.concatenate(lines, axis=1)

    loads.wait_whole(7)

    @pl.loop(0, 3)
    def _(c):
        loads.wait_part(0, c)
        enter(guess_in, field, c)
        local_sum(field, c)


    for at in range(2, len(loads.staged)):
        if at != 7:
            loads.wait_whole(at)
    upper_edge = jnp.full((1, 128), upper[0], jnp.float32)
    lower_edge = lower_ratio[0] * upper_edge
    center = (upper_edge + lower_edge) / 2.0
    radius = (upper_edge - lower_edge) / 2.0
    sigma_ratio = center / radius
    none_row = jnp.zeros((1, 128), jnp.float32)
    one_row = jnp.ones((1, 128), jnp.float32)
    coef[0, 0] = none_row
    coef[1, 0] = none_row
    coef[2, 0] = one_row
    for sweep in range(SWEEPS):
        first = sweep * CHEB + 1
        coef[0, first] = none_row
        coef[1, first] = 1.0 / center
        coef[2, first] = none_row
        factor = 1.0 / sigma_ratio
        for later in range(1, CHEB):
            factor_next = 1.0 / (2.0 * sigma_ratio - factor)
            coef[0, first + later] = factor_next * factor
            coef[1, first + later] = 2.0 * factor_next / radius
            coef[2, first + later] = none_row
            factor = factor_next

    kinds = jnp.concatenate([material[:, b, :] for b in range(elems_y)], axis=0)
    tables = []
    for row in range(2):
        picked = jnp.zeros(kinds.shape, jnp.float32)
        for kind in range(lame.shape[1]):
            picked = jnp.where(kinds == kind, lame[row, kind], picked)
        tables.append(
            jnp.dot(picked, spread_in[...], precision=highest, preferred_element_type=jnp.float32)
        )
    lam_all, mu_all = tables

    @pl.loop(0, N1)
    def _(i):
        for j in range(N1):
            lam_w[i, j] = lam_all * weight_in[i, j]
            mu_w[i, j] = mu_all * weight_in[i, j]

    @pl.loop(0, 3 * N1, unroll=N1)
    def _(at):
        c = at // N1
        i = at % N1
        pieces = []
        for j in range(N1):
            own = own_in[c, i, j]
            pieces.append(lam_w[i, j] * own + mu_w[i, j] * (sum_in[i, j] + own))
        high, low = halves(jnp.concatenate(pieces, axis=0))
        summed = jnp.dot(
            jnp.concatenate([high, low], axis=1), join_in[...], preferred_element_type=jnp.float32
        )
        inverse[c, i] = summed.reshape(N1, cols, 128)

    for c in range(3):
        local_sum(inverse, c)

    weights, derivative, _, own, second = element_tables()
    edge = float(np.float32(1.0 / weights[0]))
    groups = [slice(8 * h, 8 * h + 8) for h in range(cols // 8)]

    def product(parts, matrix):
        both = jnp.dot(
            jnp.concatenate(parts, axis=1), matrix[...], preferred_element_type=jnp.float32
        )
        return (both[:, :128] + both[:, 128:]).reshape(full)

    def forward(c, j, values):
        if c == 2:
            own_z[:, j] = product(halves(values.reshape(flat)), own_mat)
        for rows in groups:
            lines = [values[i, rows] for i in range(N1)]
            outs = apply_pairs(own, lines, -1) if c == 0 else apply_pairs(second, lines, 1)
            for i in range(N1):
                along_x[c, i, j, rows] = outs[i]

    def advance(c, step):
        alpha = coef[0, step]
        beta = coef[1, step]

        @pl.loop(0, N1, unroll=N1)
        def _(j):
            new = alpha * change[c, :, j] + beta * (inverse[c, :, j] * resid[c, :, j])
            change[c, :, j] = new
            new = field[c, :, j] + new
            field[c, :, j] = new
            forward(c, j, new)

    def sheet(i, edge_x):
        lines_y = []
        lines_v = []
        lines_z = []
        lines_t = []
        edge_z = edge_in[...]
        for rows in groups:
            u_x = [field[0, i, j, rows] for j in range(N1)]
            u_y = [field[1, i, j, rows] for j in range(N1)]
            u_z = [field[2, i, j, rows] for j in range(N1)]
            g_y = apply_pairs(own, u_y, -1)
            second_x = apply_pairs(second, u_x, 1)
            second_z = apply_pairs(second, u_z, 1)
            extra_y = []
            t_y = []
            group_v = []
            group_z = []
            group_t = []
            for j in range(N1):
                lam = lam_w[i, j, rows]
                mu = mu_w[i, j, rows]
                g_x = along_x[0, i, j, rows]
                g_z = own_z[i, j, rows]
                g_xy = g_x + g_y[j]
                e_z = edge_z * u_z[j]
                away_z = g_z - e_z
                shrink = g_xy + away_z
                own_x = g_x
                own_y = g_y[j]
                left = second_x[j]
                right = along_x[1, i, j, rows]
                if edge_x is not None:
                    e_x = edge_x * u_x[j]
                    shrink = shrink - e_x
                    own_x = g_x - (e_x + e_x)
                    left = left + edge_x * (g_y[j] + g_z)
                if j in (0, DEG):
                    edge_y = -edge if j == 0 else edge
                    e_y = edge_y * u_y[j]
                    shrink = shrink - e_y
                    own_y = g_y[j] - (e_y + e_y)
                    right = right + edge_y * (g_x + g_z)
                base = lam * shrink + mu * (g_xy + g_z)
                stress_x[i, j, rows] = base + mu * own_x
                part_x[i, j, rows] = mu * left
                t_y.append(base + mu * own_y)
                extra_y.append(mu * right)
                group_v.append(mu * u_y[j])
                group_t.append(base + mu * (away_z - e_z))
                group_z.append(mu * ((along_x[2, i, j, rows] + second_z[j]) + edge_z * g_xy))
            back_y = apply_pairs(-derivative.T, t_y, -1)
            lines_y.append([back_y[j] + extra_y[j] for j in range(N1)])
            lines_v.append(group_v)
            lines_z.append(group_z)
            lines_t.append(group_t)

        def stacked(lines):
            return jnp.concatenate([lines[h][j] for j in range(N1) for h in range(len(groups))], axis=0)

        parts = halves(stacked(lines_y)) + halves(stacked(lines_v))
        resid[1, i] = source[1, i] - product(parts, second_mat)
        parts = halves(stacked(lines_z)) + halves(stacked(lines_t))
        resid[2, i] = source[2, i] - product(parts, back_mat)

    def closing(j):
        lines_x = []
        lines_v = []
        for rows in groups:
            back_x = apply_pairs(-derivative.T, [stress_x[i, j, rows] for i in range(N1)], -1)
            lines_x.append([part_x[i, j, rows] + back_x[i] for i in range(N1)])
            lines_v.append([mu_w[i, j, rows] * field[0, i, j, rows] for i in range(N1)])

        def stacked(lines):
            return jnp.concatenate([lines[h][i] for i in range(N1) for h in range(len(groups))], axis=0)

        parts = halves(stacked(lines_x)) + halves(stacked(lines_v))
        resid[0, :, j] = source[0, :, j] - product(parts, second_mat)

    def volume(step, slot):
        for c in (1, 2, 0):
            advance(c, step)

        @pl.loop(1, DEG, unroll=UNROLL)
        def _(i):
            sheet(i, None)

        for side in range(2):
            sheet(side * DEG, edge if side else -edge)

        wait_for(slot, along_y)

        @pl.loop(0, N1, unroll=N1)
        def _(j):
            closing(j)

    arrived = (arrived_x, arrived_y)
    scale = (scale_x, scale_y)
    per_side = (elems_y, elems_x)
    ring = 2 * elems_x
    windows = (slice(0, ring), slice(cols - ring, cols))
    row_id = lax.broadcasted_iota(jnp.int32, (cols, 128), 0)
    ring_id = [lax.broadcasted_iota(jnp.int32, (2 * size, 128), 0) for size in per_side]
    low_side = [ring_id[axis] < per_side[axis] for axis in range(2)]
    place_t = [ring_id[axis] % per_side[axis] for axis in range(2)]
    lines_low = pl.ds(0, elems_y, stride=elems_x)
    lines_high = pl.ds(last_x, elems_y, stride=elems_x)

    def by_side(axis, low, high):
        return jnp.where(low_side[axis], low, high)

    def rank_tables():
        for axis in range(2):
            for p in range(N1):
                rows = []
                for f in (0, DEG):
                    others = [k for k in range(N1) if k != f]
                    chain = sum(derivative[k, p] * weights[k] * own[k, f] for k in others)
                    away = float(p != f)
                    heavy = away * weights[p]
                    rows.append((away * derivative[f, p], -away * chain, heavy * second[p, f], heavy * own[p, f]))
                for kind in range(4):
                    low, high = (float(np.float32(row[kind])) for row in rows)
                    if axis == 0:
                        col = row_id % elems_x
                        rank_x[kind, p] = jnp.where(col == 0, low, jnp.where(col == last_x, high, 0.0))
                    else:
                        rank_y[0, kind, p] = by_side(1, low, 0.0)
                        rank_y[1, kind, p] = by_side(1, 0.0, high)

    def gather_x(ref, c, low, high, dst, at):
        half = per_side[0]
        for t in range(N1):
            dst[at, t, 0:half, :] = ref[c, low, t, lines_low, :]
            dst[at, t, half : 2 * half, :] = ref[c, high, t, lines_high, :]

    def face_y(ref, c, t):
        return jnp.where(low_side[1], ref[c, t, 0, windows[0]], ref[c, t, DEG, windows[1]])

    def add_y(ref, c, t, value):
        ref[c, t, 0, windows[0]] = ref[c, t, 0, windows[0]] + by_side(1, value, 0.0)
        ref[c, t, DEG, windows[1]] = ref[c, t, DEG, windows[1]] + by_side(1, 0.0, value)

    def add_x(ref, c, t):
        half = per_side[0]
        ref[c, 0, t, lines_low, :] = ref[c, 0, t, lines_low, :] + delta[c, t, 0:half, :]
        ref[c, DEG, t, lines_high, :] = ref[c, DEG, t, lines_high, :] + delta[c, t, half : 2 * half, :]

    def face_weights():
        half = per_side[0]
        for kind, ref in enumerate((lam_w, mu_w)):
            for t in range(N1):
                face_w[0, kind, t, 0:half, :] = ref[0, t, lines_low, :]
                face_w[0, kind, t, half : 2 * half, :] = ref[0, t, lines_high, :]
                face_w[1, kind, t] = jnp.where(low_side[1], ref[0, t, windows[0]], ref[0, t, windows[1]])

    def face_scales():
        for c in range(3):
            gather_x(inverse, c, 0, DEG, scale_x, c)
            for t in range(N1):
                scale_y[c, t] = face_y(inverse, c, t)

    def arrive_y(slot):
        for c in range(3):
            arrived_y[c, :, 0:elems_x, :] = recv_y[slot, 0, c]
            arrived_y[c, :, elems_x:ring, :] = recv_y[slot, 1, c]

    def arrive_x(slot):
        half = per_side[0]
        for c in range(3):
            arrived_x[c, :, 0:half, :] = recv_x[slot, 0, c]
            arrived_x[c, :, half : 2 * half, :] = recv_x[slot, 1, c]
            for a in range(2):
                for b in range(2):
                    at = a * half + b * (half - 1)
                    arrived_x[c, b * DEG, at : at + 1, :] += (
                        recv_c[slot, 2 * a + b, c] + recv_y[slot, b, c, a * DEG, a * last_x : a * last_x + 1, :]
                    )

    def send_rim(slot):
        half = per_side[0]
        for c in range(3):
            low = rim[c, 0]
            high = rim[c, DEG]
            rim[c, 0] = low + jnp.where(place_t[0] >= 1, pltpu.roll(high, 1, 0), 0.0)
            rim[c, DEG] = high + jnp.where(place_t[0] < half - 1, pltpu.roll(low, 2 * half - 1, 0), 0.0)
            send_x[slot, 0, c] = rim[c, :, 0:half, :]
            send_x[slot, 1, c] = rim[c, :, half : 2 * half, :]
            for a in range(2):
                for b in range(2):
                    at = a * half + b * (half - 1)
                    send_c[slot, 2 * a + b, c] = rim[c, b * DEG, at : at + 1, :]
        start_all(slot, along_x_or_corner)

    def correct(axis, step, slot):
        normal, side = axis, 1 - axis
        beta = coef[1, step]
        plain = coef[2, step]
        edge_z = edge_in[...]
        edge_n = by_side(axis, -edge, edge)
        own_f = by_side(axis, float(np.float32(own[0, 0])), float(np.float32(own[DEG, DEG])))
        second_f = float(np.float32(second[0, 0]))
        per_w = float(np.float32(1.0 / weights[0]))
        chain_f = [sum(derivative[k, f] * weights[k] * own[k, f] for k in range(N1) if k != f) for f in (0, DEG)]
        first_f = by_side(axis, float(np.float32(derivative[0, 0])), float(np.float32(derivative[DEG, DEG])))
        then_f = by_side(axis, *(float(np.float32(-value)) for value in chain_f))
        size = 2 * per_side[axis]
        half = per_side[0]
        d = [[None] * N1 for _ in range(3)]
        for c in range(3):
            for t in range(N1):
                value = (plain + beta * scale[axis][c, t]) * arrived[axis][c, t]
                if axis == 1 and t in (0, DEG):
                    value = jnp.where(place_t[1] == (0 if t == 0 else last_x), 0.0, value)
                d[c][t] = value
        d_n, d_t, d_z = d[normal], d[side], d[2]

        def stack(lines):
            return jnp.concatenate(lines, axis=0)

        def joint(parts, matrix, count):
            both = jnp.dot(
                jnp.concatenate(parts, axis=1), matrix[...], preferred_element_type=jnp.float32
            )
            return (both[:, :128] + both[:, 128:]).reshape(count, N1, size, 128)

        g_z = joint(halves(stack(d_z)), own_mat, 1)[0]
        g_t = apply_pairs(own, d_t, -1)
        second_n = apply_pairs(second, d_n, 1)
        second_z = apply_pairs(second, d_z, 1)
        t_n, t_t, t_z, left, v_n, v_t, extra, f_z = [[] for _ in range(8)]
        stiff, mixed, mixed_t, mixed_z, one_t, one_z = [[] for _ in range(6)]
        for t in range(N1):
            lam = face_w[axis, 0, t]
            mu = face_w[axis, 1, t]
            g_n = own_f * d_n[t]
            g_nt = g_n + g_t[t]
            e_n = edge_n * d_n[t]
            e_z = edge_z * d_z[t]
            away_z = g_z[t] - e_z
            shrink = (g_nt + away_z) - e_n
            own_t = g_t[t]
            right = second_f * d_t[t]
            mu_d = mu * d_n[t]
            mu_in = per_w * mu_d
            mixed.append(per_w * (lam * d_n[t]) + mu_in)
            stiff.append(mixed[t] + mu_in)
            if t in (0, DEG):
                edge_t = -edge if t == 0 else edge
                e_t = edge_t * d_t[t]
                shrink = shrink - e_t
                own_t = own_t - (e_t + e_t)
                right = right + edge_t * (g_n + g_z[t])
                mixed_t.append(edge_t * mu_in)
            else:
                mixed_t.append(None)
            base = lam * shrink + mu * (g_nt + g_z[t])
            t_n.append(base + mu * (g_n - (e_n + e_n)))
            t_t.append(base + mu * own_t)
            t_z.append(base + mu * (away_z - e_z))
            left.append(mu * (second_n[t] + edge_n * (g_t[t] + g_z[t])))
            v_n.append(mu_d)
            v_t.append(mu * d_t[t])
            extra.append(mu * right)
            f_z.append(mu * ((second_f * d_z[t] + second_z[t]) + edge_z * g_nt))
            mixed_z.append(edge_z * mu_in)
            one_t.append(per_w * v_t[t])
            one_z.append(per_w * (mu * d_z[t]))
        back_t = apply_pairs(-derivative.T, t_t, -1)
        back_m = apply_pairs(-derivative.T, mixed, -1)
        f_t = [back_t[t] + extra[t] for t in range(N1)]
        two_t = [back_m[t] if mixed_t[t] is None else back_m[t] + mixed_t[t] for t in range(N1)]
        parts = halves(stack(left + f_t)) + halves(stack(v_n + v_t))
        faces = joint(parts, second_mat, 2)
        parts = halves(stack(f_z)) + halves(stack(t_z))
        face_z = joint(parts, back_mat, 1)[0]

        def joined(lines, count):
            return jnp.dot(
                jnp.concatenate(halves(stack(lines)), axis=1),
                exact_mat[...],
                preferred_element_type=jnp.float32,
            ).reshape(count, N1, size, 128)

        along_n = joined(t_n + stiff, 2)
        away = joined(one_t + two_t + one_z, 3)
        parts = halves(stack(mixed_z)) + halves(stack(mixed))
        upright = joint(parts, back_mat, 1)[0]
        at_face = {normal: faces[0], side: faces[1], 2: face_z}
        if axis == 0:
            for c in range(3):
                gather_x(resid, c, 0, DEG, rim, c)
        for c in range(3):
            for t in range(N1):
                value = at_face[c][t]
                if c == normal:
                    value = value + (then_f * along_n[1, t] - first_f * along_n[0, t])
                if axis == 0:
                    left_over = rim[c, t] - value
                    rim[c, t] = left_over
                    delta[c, t] = left_over
                else:
                    add_y(resid, c, t, -value)
        if axis == 0:
            for c in range(3):
                for t in range(N1):
                    resid[c, 0, t, lines_low, :] = delta[c, t, 0:half, :]
                    resid[c, DEG, t, lines_high, :] = delta[c, t, half : 2 * half, :]
            send_rim(slot)
        pairs = {normal: (0, -along_n[0], along_n[1]), side: (2, away[0], away[1]), 2: (2, away[2], upright)}
        for c in range(3):
            for t in range(N1):
                if axis == 0:
                    delta[c, t] = d[c][t]
                    add_x(field, c, t)
                    add_x(change, c, t)
                else:
                    add_y(field, c, t, d[c][t])
                    add_y(change, c, t, d[c][t])
        for t in range(N1):
            for c in range(3):
                kind, first, then = pairs[c]
                if axis == 0:
                    for k, value in enumerate((first[t], then[t])):
                        narrow[2 * c + k, t] = value
                        wide[2 * c + k, t, lines_low, :] = narrow[2 * c + k, t, 0:half, :]
                        wide[2 * c + k, t, lines_high, :] = narrow[2 * c + k, t, half : 2 * half, :]
                    first_t, then_t = wide[2 * c, t], wide[2 * c + 1, t]
                    for p in range(N1):
                        change_by = rank_x[kind, p] * first_t + rank_x[kind + 1, p] * then_t
                        resid[c, p, t] = resid[c, p, t] - change_by
                else:
                    for p in range(N1):
                        for w, rows in enumerate(windows):
                            change_by = rank_y[w, kind, p] * first[t] + rank_y[w, kind + 1, p] * then[t]
                            resid[c, t, p, rows] = resid[c, t, p, rows] - change_by

    @pl.loop(0, 3)
    def _(c):
        loads.wait_part(1, c)
        enter(source_in, source, c)

    rank_tables()
    face_weights()
    for ref in (scale_x, scale_y, wide):
        ref[...] = jnp.zeros(ref.shape, jnp.float32)

    for c in range(3):

        @pl.loop(0, N1)
        def _(i):
            change[c, i] = zeros_big
            resid[c, i] = zeros_big

    for c in range(3):
        fill(field, 0, c)
        fill(inverse, 2, c)

    pl.semaphore_wait(barrier, len(partners))

    start_all(0, every)
    start_all(2, every)

    @pl.loop(0, steps + 1)
    def _(step):
        slot = step % 2
        volume(step, slot)
        arrive_y(slot)
        correct(1, step, 1 - slot)
        wait_for(slot, along_x_or_corner)
        arrive_x(slot)
        correct(0, step, 1 - slot)

        @pl.loop(0, 3)
        def _(c):
            local_sum(resid, c)
            fill_y(resid, 1 - slot, c)

        start_all(1 - slot, along_y)

        @pl.when(step == 0)
        def _():
            wait_for(2, every)

            @pl.loop(0, 3)
            def _(c):
                collect(inverse, 2, c)

                @pl.loop(0, N1)
                def _(i):
                    inverse[c, i] = 1.0 / inverse[c, i]

            face_scales()

    @pl.loop(0, 3)
    def _(c):
        leave(field, smoothed_out, c)

    @pl.loop(0, 3)
    def _(c):
        leave(resid, residual_out, c)

    edge_lines[...] = jnp.zeros(edge_lines.shape, jnp.float32)
    slot = (steps + 1) % 2
    wait_for(slot, every)
    arrive_y(slot)
    arrive_x(slot)
    for c in range(3):
        for t in range(DEG):
            edge_lines[c, 0, pl.ds(t, elems_y, stride=DEG), :] = arrived_x[c, t, 0:elems_y, :]
            edge_lines[c, 1, pl.ds(t, elems_x, stride=DEG), :] = arrived_y[c, t, 0:elems_x, :]
        edge_lines[c, 1, 0:1, :] = jnp.zeros((1, 128), jnp.float32)
    depth = edge_lines.shape[2]
    parts = halves(edge_lines[...].reshape(6 * depth, 128))
    found = jnp.dot(
        jnp.concatenate(parts, axis=1), select_in[...], preferred_element_type=jnp.float32
    )
    patch_out[...] = found.reshape(patch_out.shape)


def finish(nodes_z, nodes_x, nodes_y, smoothed_in, residual_in, patch_in, smoothed_out, residual_out, held, put_sem):
    def put(at, source, target, c):
        return pltpu.make_async_copy(source.at[c], target.at[c], put_sem.at[at, c])

    for c in range(3):
        put(0, smoothed_in, smoothed_out, c).start()
    for c in range(3):
        pieces = [patch_in[c, 0, y : y + 1, 0:nodes_z] for y in range(nodes_y)]
        held[c] = residual_in[c]
        held[c, 0:1, :] = held[c, 0:1, :] + jnp.concatenate(pieces, axis=1)
        held[c, :, 0:nodes_z] = held[c, :, 0:nodes_z] + patch_in[c, 1, 0:nodes_x, 0:nodes_z]
        put(1, held, residual_out, c).start()
    for c in range(3):
        put(0, smoothed_in, smoothed_out, c).wait()
        put(1, held, residual_out, c).wait()


def z_join(blocks, clamped):
    nodes = DEG * blocks + 1
    gather = np.zeros((nodes, blocks * N1))
    for element in range(blocks):
        for k in range(N1):
            gather[DEG * element + k, element * N1 + k] = 1.0
    if clamped:
        gather[0] = 0.0
        gather[nodes - 1] = 0.0
    return gather.T @ gather


def local(right_side, guess, material, lame, upper, lower_ratio):
    elems_x, elems_y, elems_z = material.shape
    cols = elems_x * elems_y
    lanes = N1 * elems_z
    nodes_z = DEG * elems_z - 1
    weights_np, derivative_np, ratio_np, own_np_1, second_np = element_tables()
    eye_z = np.eye(elems_z)
    join_np = z_join(elems_z, True)
    joined = join_np.astype(jnp.bfloat16)

    def exact_pair(matrix):
        high, low = np_halves(matrix)
        none = np.zeros_like(high)
        return [[high, low], [high, none]]

    exact_join = [[joined, np.zeros_like(joined)]] * 2
    own_mat = jnp.asarray(np.block(exact_pair(np.kron(eye_z, own_np_1.T))))
    back_np = np.kron(eye_z, derivative_np) @ join_np
    back_mat = jnp.asarray(np.block(exact_join + exact_pair(-back_np)))
    scaled_np = np.kron(eye_z, second_np) @ join_np
    second_mat = jnp.asarray(np.block(exact_join + exact_pair(scaled_np)))
    exact_mat = jnp.asarray(np.concatenate([joined, joined], axis=0))
    edge_np = np.zeros((1, lanes))
    edge_np[0, 0::N1] = -1.0 / weights_np[0]
    edge_np[0, DEG::N1] = 1.0 / weights_np[DEG]
    edge_in = jnp.asarray(edge_np, jnp.float32)
    all_join = z_join(elems_z, False).astype(jnp.bfloat16)
    join_in = jnp.asarray(np.concatenate([all_join, all_join], axis=0))

    weights_z = np.tile(weights_np, elems_z)
    ratio_z = np.tile(ratio_np, elems_z)
    weight_np = weights_np[:, None, None] * weights_np[None, :, None] * weights_z
    shape_w = (N1, N1, lanes)
    own_x = np.broadcast_to(ratio_np[:, None, None], shape_w)
    own_y = np.broadcast_to(ratio_np[None, :, None], shape_w)
    own_z = np.broadcast_to(ratio_z, shape_w)
    own_np = np.stack([own_x, own_y, own_z])
    weight_in = jnp.asarray(weight_np[:, :, None], jnp.float32)
    own_in = jnp.asarray(own_np[:, :, :, None], jnp.float32)
    sum_in = jnp.asarray((own_x + own_y + own_z)[:, :, None], jnp.float32)

    gather_np = clamped_gather(elems_z)
    nodes_z = gather_np.shape[0]
    owned_np = gather_np.copy()
    owned_np[:, DEG::N1] = 0.0
    enter_np = np.zeros((lanes, lanes))
    enter_np[:nodes_z] = gather_np
    leave_np = np.zeros((lanes, lanes))
    leave_np[:, :nodes_z] = owned_np.T
    gather_in = jnp.asarray(np.concatenate([enter_np, enter_np], axis=0).astype(jnp.bfloat16))
    select_in = jnp.asarray(np.concatenate([leave_np, leave_np], axis=0).astype(jnp.bfloat16))
    spread_in = jnp.asarray(np.kron(eye_z, np.ones((1, N1))), dtype=jnp.float32)

    pad_x = -(-DEG * elems_x // 8) * 8
    whole = (3, N1, N1, cols, lanes)
    smem = pl.BlockSpec(memory_space=pltpu.SMEM)
    big = pltpu.VMEM(whole, jnp.float32)
    small = pltpu.VMEM((N1, N1, cols, lanes), jnp.float32)
    ring = 2 * elems_x
    face_a = pltpu.VMEM((3, N1, 2 * elems_y, lanes), jnp.float32)
    face_b = pltpu.VMEM((3, N1, ring, lanes), jnp.float32)
    edge_size = -(-DEG * max(elems_x, elems_y) // 8) * 8
    lines = pltpu.VMEM((DEG * elems_y, pad_x, lanes), jnp.float32)
    face_x = pltpu.VMEM((SLOTS, 2, 3, N1, elems_y, lanes), jnp.float32)
    face_y = pltpu.VMEM((SLOTS, 2, 3, N1, elems_x, lanes), jnp.float32)
    corner = pltpu.VMEM((SLOTS, 4, 3, 1, lanes), jnp.float32)
    shape = jax.ShapeDtypeStruct(guess.shape, jnp.float32)

    operands = [
        guess,
        right_side,
        material,
        weight_in,
        own_in,
        sum_in,
        spread_in,
        gather_in,
        select_in,
        edge_in,
        own_mat,
        back_mat,
        second_mat,
        exact_mat,
        join_in,
    ]
    number = len(operands)

    def kernel(*refs):
        scalars, places, outs = refs[:3], refs[3 : 3 + number], refs[3 + number : 6 + number]
        staged, rest = refs[6 + number : 6 + 2 * number], refs[6 + 2 * number :]
        loads = Loads(places, staged, *rest[:2])
        smoother_kernel(SWEEPS * CHEB, elems_x, elems_y, *scalars, loads, *outs, *rest[2:])

    away = pl.BlockSpec(memory_space=pl.ANY)
    vmem = pl.BlockSpec(memory_space=pltpu.VMEM)
    operands = [pltpu.with_memory_space_constraint(operand, pltpu.HBM) for operand in operands]
    patch_shape = (3, 2, edge_size, lanes)
    results = pl.pallas_call(
        kernel,
        out_shape=(shape, shape, jax.ShapeDtypeStruct(patch_shape, jnp.float32)),
        in_specs=[smem] * 3 + [away] * number,
        out_specs=(vmem, vmem, vmem),
        scratch_shapes=[pltpu.VMEM(operand.shape, operand.dtype) for operand in operands]
        + [pltpu.SemaphoreType.DMA((2, 3)), pltpu.SemaphoreType.DMA((number,))]
        + [pltpu.VMEM((3, SWEEPS * CHEB + 1, 1, lanes), jnp.float32)]
        + [big] * 3
        + [small] * 2
        + [big] * 3
        + [small] * 3
        + [face_a, face_b] * 2
        + [pltpu.VMEM((4, N1, cols, lanes), jnp.float32)]
        + [pltpu.VMEM((2, 4, N1, ring, lanes), jnp.float32)]
        + [face_a] * 2
        + [pltpu.VMEM((6, N1, 2 * elems_y, lanes), jnp.float32)]
        + [pltpu.VMEM((6, N1, cols, lanes), jnp.float32)]
        + [pltpu.VMEM((2, 2, N1, ring, lanes), jnp.float32)]
        + [pltpu.VMEM(patch_shape, jnp.float32)]
        + [lines] * 2
        + [face_x, face_y, corner] * 2
        + [pltpu.SemaphoreType.DMA((SLOTS, 8))] * 2,
        compiler_params=pltpu.CompilerParams(
            collective_id=0, has_side_effects=True, vmem_limit_bytes=VMEM_BYTES
        ),
    )(pltpu.with_memory_space_constraint(lame, pltpu.HBM), upper, lower_ratio, *operands)

    def finish_kernel(*refs):
        finish(nodes_z, DEG * elems_x, DEG * elems_y, *refs)

    return pl.pallas_call(
        finish_kernel,
        out_shape=(shape, shape),
        in_specs=[vmem] * 3,
        out_specs=(away, away),
        scratch_shapes=[pltpu.VMEM(guess.shape, jnp.float32), pltpu.SemaphoreType.DMA((2, 3))],
        compiler_params=pltpu.CompilerParams(vmem_limit_bytes=VMEM_BYTES // 2),
    )(*results)


def solution(mesh):
    placed = (P(None, "gx", "gy"), P(None, "gx", "gy"), P("gx", "gy", None), P(), P(), P())
    return jax.shard_map(
        local,
        mesh=mesh,
        in_specs=placed,
        out_specs=(P(None, "gx", "gy"), P(None, "gx", "gy")),
        check_vma=False,
    )
```

```python
import jax
import jax.numpy as jnp
import numpy as np
from jax import lax
from jax.experimental import pallas as pl
from jax.experimental.pallas import tpu as pltpu
from jax.sharding import PartitionSpec as P

DEG = 7
SWEEPS = 2
CHEB = 3


highest = lax.Precision.HIGHEST


def legendre_pair(points, degree):
    prev_poly = points * 0.0 + 1.0
    this_poly = points * 1.0
    for order in range(2, degree + 1):
        next_poly = ((2 * order - 1) * points * this_poly - (order - 1) * prev_poly) / order
        prev_poly = this_poly
        this_poly = next_poly
    return (this_poly, prev_poly)


def gll_tables(degree):
    count = degree + 1
    points = -np.cos(np.pi * np.arange(count) / degree)
    for newton_step in range(60):
        this_poly, prev_poly = legendre_pair(points, degree)
        points = points - (points * this_poly - prev_poly) / (count * this_poly)
    values, unused_poly = legendre_pair(points, degree)
    weights = 2.0 / (degree * (degree + 1) * values**2)
    identity_np = np.eye(count)
    spacing = points[:, None] - points[None, :] + identity_np
    derivative = values[:, None] / (values[None, :] * spacing) * (1.0 - identity_np)
    derivative[0, 0] = -degree * (degree + 1) / 4.0
    derivative[degree, degree] = degree * (degree + 1) / 4.0
    stiff_ratio = (weights[:, None] * derivative**2).sum(0) / weights
    return (weights, derivative, stiff_ratio)


def clamped_gather(blocks):
    free_nodes = DEG * blocks - 1
    selector = np.zeros((free_nodes, blocks * (DEG + 1)), np.float32)
    for element in range(blocks):
        for node_idx in range(DEG + 1):
            target = DEG * element + node_idx - 1
            if 0 <= target < free_nodes:
                selector[target, element * (DEG + 1) + node_idx] = 1.0
    return selector


N1 = DEG + 1
SLOTS = 3
UNROLL = 6
VMEM_BYTES = 36 * 1024 * 1024


def halves(value):
    high = value.astype(jnp.bfloat16)
    low = (value - high.astype(jnp.float32)).astype(jnp.bfloat16)
    return high, low


def np_halves(matrix):
    high = np.asarray(matrix, np.float32).astype(jnp.bfloat16)
    low = (np.asarray(matrix, np.float64) - high.astype(np.float64)).astype(jnp.bfloat16)
    return high, low


def apply_pairs(matrix, values, parity):
    half = N1 // 2
    even = [values[i] + values[DEG - i] for i in range(half)]
    odd = [values[i] - values[DEG - i] for i in range(half)]
    outs = [None] * N1
    for p in range(half):
        plus = None
        minus = None
        for i in range(half):
            by_even = float(np.float32((matrix[p, i] + matrix[p, DEG - i]) / 2))
            by_odd = float(np.float32((matrix[p, i] - matrix[p, DEG - i]) / 2))
            plus = by_even * even[i] if plus is None else plus + by_even * even[i]
            minus = by_odd * odd[i] if minus is None else minus + by_odd * odd[i]
        outs[p] = minus + plus
        outs[DEG - p] = plus - minus if parity > 0 else minus - plus
    return outs


def element_tables():
    weights, derivative, ratio = gll_tables(DEG)
    own = derivative.T * weights[None, :] / weights[:, None]
    second = own @ derivative
    return weights, derivative, ratio, own, second


class Loads:
    def __init__(self, places, staged, part_sem, whole_sem):
        self.places = places
        self.staged = staged
        self.part_sem = part_sem
        self.whole_sem = whole_sem

    def part(self, at, c):
        return pltpu.make_async_copy(
            self.places[at].at[c], self.staged[at].at[c], self.part_sem.at[at, c]
        )

    def whole(self, at):
        return pltpu.make_async_copy(self.places[at], self.staged[at], self.whole_sem.at[at])

    def start(self):
        self.whole(7).start()
        for c in range(3):
            self.part(0, c).start()
        for at in range(2, len(self.places)):
            if at != 7:
                self.whole(at).start()
        for c in range(3):
            self.part(1, c).start()

    def wait_part(self, at, c):
        self.part(at, c).wait()

    def wait_whole(self, at):
        self.whole(at).wait()


def smoother_kernel(
    steps,
    elems_x,
    elems_y,
    lame,
    upper,
    lower_ratio,
    loads,
    smoothed_out,
    residual_out,
    patch_out,
    coef,
    field,
    resid,
    source,
    lam_w,
    mu_w,
    inverse,
    change,
    along_x,
    own_z,
    stress_x,
    part_x,
    arrived_x,
    arrived_y,
    scale_x,
    scale_y,
    rank_x,
    rank_y,
    rim,
    delta,
    narrow,
    wide,
    face_w,
    edge_lines,
    flat_a,
    flat_b,
    send_x,
    send_y,
    send_c,
    recv_x,
    recv_y,
    recv_c,
    send_sem,
    recv_sem,
):
    loads.start()
    (guess_in, source_in, material, weight_in, own_in, sum_in, spread_in, gather_in) = loads.staged[:8]
    (select_in, edge_in, own_mat, back_mat, second_mat, exact_mat, join_in) = loads.staged[8:]
    cols = elems_x * elems_y
    size_x = lax.axis_size("gx")
    size_y = lax.axis_size("gy")
    me_x = lax.axis_index("gx")
    me_y = lax.axis_index("gy")
    near_x = (lax.rem(me_x + size_x - 1, size_x), lax.rem(me_x + 1, size_x))
    near_y = (lax.rem(me_y + size_y - 1, size_y), lax.rem(me_y + 1, size_y))
    partners = [(near_x[0], me_y), (near_x[1], me_y), (me_x, near_y[0]), (me_x, near_y[1])]
    partners += [(near_x[a], near_y[b]) for a in range(2) for b in range(2)]

    barrier = pltpu.get_barrier_semaphore()
    for partner in partners:
        pl.semaphore_signal(
            barrier, inc=1, device_id=partner, device_id_type=pl.DeviceIdType.MESH
        )

    def copy_of(slot, d):
        if d < 2:
            src, dst = send_x.at[slot, d], recv_x.at[slot, 1 - d]
        elif d < 4:
            src, dst = send_y.at[slot, d - 2], recv_y.at[slot, 3 - d]
        else:
            src, dst = send_c.at[slot, d - 4], recv_c.at[slot, 7 - d]
        mirror = (1, 0, 3, 2, 7, 6, 5, 4)[d]
        return pltpu.make_async_remote_copy(
            src_ref=src,
            dst_ref=dst,
            send_sem=send_sem.at[slot, d],
            recv_sem=recv_sem.at[slot, mirror],
            device_id=partners[d],
            device_id_type=pl.DeviceIdType.MESH,
        )

    def start_all(slot, kinds):
        for d in kinds:
            copy_of(slot, d).start()

    def wait_for(slot, kinds):
        for d in kinds:
            copy_of(slot, d).wait()

    along_y = (2, 3)
    along_x_or_corner = (0, 1, 4, 5, 6, 7)
    every = range(8)

    rows = lax.broadcasted_iota(jnp.int32, (N1 * cols, 128), 0) % cols
    row_x = rows % elems_x
    inner_low_y = rows >= elems_x
    inner_high_y = rows < cols - elems_x
    inner_low_x = row_x >= 1
    inner_high_x = row_x < elems_x - 1
    last_x = elems_x - 1
    last_y = cols - elems_x
    flat = (N1 * cols, 128)
    full = (N1, cols, 128)

    def local_sum(ref, c):
        zero = jnp.zeros(flat, jnp.float32)
        low = ref[c, 0].reshape(flat)
        high = ref[c, DEG].reshape(flat)
        to_low = jnp.where(inner_low_x, pltpu.roll(high, 1, 0), zero)
        to_high = jnp.where(inner_high_x, pltpu.roll(low, N1 * cols - 1, 0), zero)
        ref[c, 0] = (low + to_low).reshape(full)
        ref[c, DEG] = (high + to_high).reshape(full)
        low = ref[c, :, 0].reshape(flat)
        high = ref[c, :, DEG].reshape(flat)
        to_low = jnp.where(inner_low_y, pltpu.roll(high, elems_x, 0), zero)
        to_high = jnp.where(inner_high_y, pltpu.roll(low, N1 * cols - elems_x, 0), zero)
        ref[c, :, 0] = (low + to_low).reshape(full)
        ref[c, :, DEG] = (high + to_high).reshape(full)

    def fill_y(ref, slot, c):
        send_y[slot, 0, c] = ref[c, :, 0, 0:elems_x, :]
        send_y[slot, 1, c] = ref[c, :, DEG, last_y:cols, :]

    def fill(ref, slot, c):
        fill_y(ref, slot, c)
        for b in range(elems_y):
            at = b * elems_x
            send_x[slot, 0, c, :, b : b + 1, :] = ref[c, 0, :, at : at + 1, :]
            at = b * elems_x + last_x
            send_x[slot, 1, c, :, b : b + 1, :] = ref[c, DEG, :, at : at + 1, :]
        for a in range(2):
            for b in range(2):
                at = a * last_x + b * last_y
                send_c[slot, 2 * a + b, c] = ref[c, a * DEG, b * DEG, at : at + 1, :]

    def collect(ref, slot, c):
        ref[c, :, 0, 0:elems_x, :] += recv_y[slot, 0, c]
        ref[c, :, DEG, last_y:cols, :] += recv_y[slot, 1, c]
        for b in range(elems_y):
            at = b * elems_x
            ref[c, 0, :, at : at + 1, :] += recv_x[slot, 0, c, :, b : b + 1, :]
            at = b * elems_x + last_x
            ref[c, DEG, :, at : at + 1, :] += recv_x[slot, 1, c, :, b : b + 1, :]
        for a in range(2):
            for b in range(2):
                at = a * last_x + b * last_y
                ref[c, a * DEG, b * DEG, at : at + 1, :] += recv_c[slot, 2 * a + b, c]

    nodes_x = DEG * elems_x
    nodes_y = DEG * elems_y
    nodes_z = guess_in.shape[2] // nodes_y
    pad_x = flat_a.shape[1]
    zeros_big = jnp.zeros((N1, cols, 128), jnp.float32)

    @pl.loop(0, nodes_y)
    def _(y):
        flat_a[y] = jnp.zeros((pad_x, 128), jnp.float32)
        flat_b[y] = jnp.zeros((pad_x, 128), jnp.float32)

    def through(src, dst, matrix):
        @pl.loop(0, elems_y, unroll=elems_y)
        def _(b):
            pick = pl.ds(b * DEG, DEG)
            parts = halves(src[pick].reshape(DEG * pad_x, 128))
            dst[pick] = jnp.dot(
                jnp.concatenate(parts, axis=1), matrix[...], preferred_element_type=jnp.float32
            ).reshape(DEG, pad_x, 128)

    def enter(flat_in, ref, c):
        lines = flat_in[c]
        for y in range(nodes_y):
            flat_a[y, 0:nodes_x, 0:nodes_z] = lines[:, y * nodes_z : (y + 1) * nodes_z]
        through(flat_a, flat_b, gather_in)
        ref[c, DEG] = zeros_big
        ref[c, :, DEG] = zeros_big
        for b in range(elems_y):
            for j in range(DEG):
                for i in range(DEG):
                    ref[c, i, j, b * elems_x : (b + 1) * elems_x, :] = flat_b[
                        b * DEG + j, pl.ds(i, elems_x, stride=DEG), :
                    ]

    def leave(ref, flat_out, c):
        for b in range(elems_y):
            for j in range(DEG):
                for i in range(DEG):
                    flat_b[b * DEG + j, pl.ds(i, elems_x, stride=DEG), :] = ref[
                        c, i, j, b * elems_x : (b + 1) * elems_x, :
                    ]
        through(flat_b, flat_a, select_in)
        lines = [flat_a[y, 0:nodes_x, 0:nodes_z] for y in range(nodes_y)]
        flat_out[c] = jnp.concatenate(lines, axis=1)

    loads.wait_whole(7)

    @pl.loop(0, 3)
    def _(c):
        loads.wait_part(0, c)
        enter(guess_in, field, c)
        local_sum(field, c)


    for at in range(2, len(loads.staged)):
        if at != 7:
            loads.wait_whole(at)
    upper_edge = jnp.full((1, 128), upper[0], jnp.float32)
    lower_edge = lower_ratio[0] * upper_edge
    center = (upper_edge + lower_edge) / 2.0
    radius = (upper_edge - lower_edge) / 2.0
    sigma_ratio = center / radius
    none_row = jnp.zeros((1, 128), jnp.float32)
    one_row = jnp.ones((1, 128), jnp.float32)
    coef[0, 0] = none_row
    coef[1, 0] = none_row
    coef[2, 0] = one_row
    for sweep in range(SWEEPS):
        first = sweep * CHEB + 1
        coef[0, first] = none_row
        coef[1, first] = 1.0 / center
        coef[2, first] = none_row
        factor = 1.0 / sigma_ratio
        for later in range(1, CHEB):
            factor_next = 1.0 / (2.0 * sigma_ratio - factor)
            coef[0, first + later] = factor_next * factor
            coef[1, first + later] = 2.0 * factor_next / radius
            coef[2, first + later] = none_row
            factor = factor_next

    kinds = jnp.concatenate([material[:, b, :] for b in range(elems_y)], axis=0)
    tables = []
    for row in range(2):
        picked = jnp.zeros(kinds.shape, jnp.float32)
        for kind in range(lame.shape[1]):
            picked = jnp.where(kinds == kind, lame[row, kind], picked)
        tables.append(
            jnp.dot(picked, spread_in[...], precision=highest, preferred_element_type=jnp.float32)
        )
    lam_all, mu_all = tables

    @pl.loop(0, N1)
    def _(i):
        for j in range(N1):
            lam_w[i, j] = lam_all * weight_in[i, j]
            mu_w[i, j] = mu_all * weight_in[i, j]

    @pl.loop(0, 3 * N1, unroll=N1)
    def _(at):
        c = at // N1
        i = at % N1
        pieces = []
        for j in range(N1):
            own = own_in[c, i, j]
            pieces.append(lam_w[i, j] * own + mu_w[i, j] * (sum_in[i, j] + own))
        high, low = halves(jnp.concatenate(pieces, axis=0))
        summed = jnp.dot(
            jnp.concatenate([high, low], axis=1), join_in[...], preferred_element_type=jnp.float32
        )
        inverse[c, i] = summed.reshape(N1, cols, 128)

    for c in range(3):
        local_sum(inverse, c)

    weights, derivative, _, own, second = element_tables()
    edge = float(np.float32(1.0 / weights[0]))
    groups = [slice(8 * h, 8 * h + 8) for h in range(cols // 8)]

    def product(parts, matrix):
        both = jnp.dot(
            jnp.concatenate(parts, axis=1), matrix[...], preferred_element_type=jnp.float32
        )
        return (both[:, :128] + both[:, 128:]).reshape(full)

    def forward(c, j, values):
        if c == 2:
            own_z[:, j] = product(halves(values.reshape(flat)), own_mat)
        for rows in groups:
            lines = [values[i, rows] for i in range(N1)]
            outs = apply_pairs(own, lines, -1) if c == 0 else apply_pairs(second, lines, 1)
            for i in range(N1):
                along_x[c, i, j, rows] = outs[i]

    def advance(c, step):
        alpha = coef[0, step]
        beta = coef[1, step]

        @pl.loop(0, N1, unroll=N1)
        def _(j):
            new = alpha * change[c, :, j] + beta * (inverse[c, :, j] * resid[c, :, j])
            change[c, :, j] = new
            new = field[c, :, j] + new
            field[c, :, j] = new
            forward(c, j, new)

    def sheet(i, edge_x):
        lines_y = []
        lines_v = []
        lines_z = []
        lines_t = []
        edge_z = edge_in[...]
        for rows in groups:
            u_x = [field[0, i, j, rows] for j in range(N1)]
            u_y = [field[1, i, j, rows] for j in range(N1)]
            u_z = [field[2, i, j, rows] for j in range(N1)]
            g_y = apply_pairs(own, u_y, -1)
            second_x = apply_pairs(second, u_x, 1)
            second_z = apply_pairs(second, u_z, 1)
            extra_y = []
            t_y = []
            group_v = []
            group_z = []
            group_t = []
            for j in range(N1):
                lam = lam_w[i, j, rows]
                mu = mu_w[i, j, rows]
                g_x = along_x[0, i, j, rows]
                g_z = own_z[i, j, rows]
                g_xy = g_x + g_y[j]
                e_z = edge_z * u_z[j]
                away_z = g_z - e_z
                shrink = g_xy + away_z
                own_x = g_x
                own_y = g_y[j]
                left = second_x[j]
                right = along_x[1, i, j, rows]
                if edge_x is not None:
                    e_x = edge_x * u_x[j]
                    shrink = shrink - e_x
                    own_x = g_x - (e_x + e_x)
                    left = left + edge_x * (g_y[j] + g_z)
                if j in (0, DEG):
                    edge_y = -edge if j == 0 else edge
                    e_y = edge_y * u_y[j]
                    shrink = shrink - e_y
                    own_y = g_y[j] - (e_y + e_y)
                    right = right + edge_y * (g_x + g_z)
                base = lam * shrink + mu * (g_xy + g_z)
                stress_x[i, j, rows] = base + mu * own_x
                part_x[i, j, rows] = mu * left
                t_y.append(base + mu * own_y)
                extra_y.append(mu * right)
                group_v.append(mu * u_y[j])
                group_t.append(base + mu * (away_z - e_z))
                group_z.append(mu * ((along_x[2, i, j, rows] + second_z[j]) + edge_z * g_xy))
            back_y = apply_pairs(-derivative.T, t_y, -1)
            lines_y.append([back_y[j] + extra_y[j] for j in range(N1)])
            lines_v.append(group_v)
            lines_z.append(group_z)
            lines_t.append(group_t)

        def stacked(lines):
            return jnp.concatenate([lines[h][j] for j in range(N1) for h in range(len(groups))], axis=0)

        parts = halves(stacked(lines_y)) + halves(stacked(lines_v))
        resid[1, i] = source[1, i] - product(parts, second_mat)
        parts = halves(stacked(lines_z)) + halves(stacked(lines_t))
        resid[2, i] = source[2, i] - product(parts, back_mat)

    def closing(j):
        lines_x = []
        lines_v = []
        for rows in groups:
            back_x = apply_pairs(-derivative.T, [stress_x[i, j, rows] for i in range(N1)], -1)
            lines_x.append([part_x[i, j, rows] + back_x[i] for i in range(N1)])
            lines_v.append([mu_w[i, j, rows] * field[0, i, j, rows] for i in range(N1)])

        def stacked(lines):
            return jnp.concatenate([lines[h][i] for i in range(N1) for h in range(len(groups))], axis=0)

        parts = halves(stacked(lines_x)) + halves(stacked(lines_v))
        resid[0, :, j] = source[0, :, j] - product(parts, second_mat)

    def volume(step, slot):
        for c in (1, 2, 0):
            advance(c, step)

        @pl.loop(1, DEG, unroll=UNROLL)
        def _(i):
            sheet(i, None)

        for side in range(2):
            sheet(side * DEG, edge if side else -edge)

        wait_for(slot, along_y)

        @pl.loop(0, N1, unroll=N1)
        def _(j):
            closing(j)

    arrived = (arrived_x, arrived_y)
    scale = (scale_x, scale_y)
    per_side = (elems_y, elems_x)
    ring = 2 * elems_x
    windows = (slice(0, ring), slice(cols - ring, cols))
    row_id = lax.broadcasted_iota(jnp.int32, (cols, 128), 0)
    ring_id = [lax.broadcasted_iota(jnp.int32, (2 * size, 128), 0) for size in per_side]
    low_side = [ring_id[axis] < per_side[axis] for axis in range(2)]
    place_t = [ring_id[axis] % per_side[axis] for axis in range(2)]
    lines_low = pl.ds(0, elems_y, stride=elems_x)
    lines_high = pl.ds(last_x, elems_y, stride=elems_x)

    def by_side(axis, low, high):
        return jnp.where(low_side[axis], low, high)

    def rank_tables():
        for axis in range(2):
            for p in range(N1):
                rows = []
                for f in (0, DEG):
                    others = [k for k in range(N1) if k != f]
                    chain = sum(derivative[k, p] * weights[k] * own[k, f] for k in others)
                    away = float(p != f)
                    heavy = away * weights[p]
                    rows.append((away * derivative[f, p], -away * chain, heavy * second[p, f], heavy * own[p, f]))
                for kind in range(4):
                    low, high = (float(np.float32(row[kind])) for row in rows)
                    if axis == 0:
                        col = row_id % elems_x
                        rank_x[kind, p] = jnp.where(col == 0, low, jnp.where(col == last_x, high, 0.0))
                    else:
                        rank_y[0, kind, p] = by_side(1, low, 0.0)
                        rank_y[1, kind, p] = by_side(1, 0.0, high)

    def gather_x(ref, c, low, high, dst, at):
        half = per_side[0]
        for t in range(N1):
            dst[at, t, 0:half, :] = ref[c, low, t, lines_low, :]
            dst[at, t, half : 2 * half, :] = ref[c, high, t, lines_high, :]

    def face_y(ref, c, t):
        return jnp.where(low_side[1], ref[c, t, 0, windows[0]], ref[c, t, DEG, windows[1]])

    def add_y(ref, c, t, value):
        ref[c, t, 0, windows[0]] = ref[c, t, 0, windows[0]] + by_side(1, value, 0.0)
        ref[c, t, DEG, windows[1]] = ref[c, t, DEG, windows[1]] + by_side(1, 0.0, value)

    def add_x(ref, c, t):
        half = per_side[0]
        ref[c, 0, t, lines_low, :] = ref[c, 0, t, lines_low, :] + delta[c, t, 0:half, :]
        ref[c, DEG, t, lines_high, :] = ref[c, DEG, t, lines_high, :] + delta[c, t, half : 2 * half, :]

    def face_weights():
        half = per_side[0]
        for kind, ref in enumerate((lam_w, mu_w)):
            for t in range(N1):
                face_w[0, kind, t, 0:half, :] = ref[0, t, lines_low, :]
                face_w[0, kind, t, half : 2 * half, :] = ref[0, t, lines_high, :]
                face_w[1, kind, t] = jnp.where(low_side[1], ref[0, t, windows[0]], ref[0, t, windows[1]])

    def face_scales():
        for c in range(3):
            gather_x(inverse, c, 0, DEG, scale_x, c)
            for t in range(N1):
                scale_y[c, t] = face_y(inverse, c, t)

    def arrive_y(slot):
        for c in range(3):
            arrived_y[c, :, 0:elems_x, :] = recv_y[slot, 0, c]
            arrived_y[c, :, elems_x:ring, :] = recv_y[slot, 1, c]

    def arrive_x(slot):
        half = per_side[0]
        for c in range(3):
            arrived_x[c, :, 0:half, :] = recv_x[slot, 0, c]
            arrived_x[c, :, half : 2 * half, :] = recv_x[slot, 1, c]
            for a in range(2):
                for b in range(2):
                    at = a * half + b * (half - 1)
                    arrived_x[c, b * DEG, at : at + 1, :] += (
                        recv_c[slot, 2 * a + b, c] + recv_y[slot, b, c, a * DEG, a * last_x : a * last_x + 1, :]
                    )

    def send_rim(slot):
        half = per_side[0]
        for c in range(3):
            low = rim[c, 0]
            high = rim[c, DEG]
            rim[c, 0] = low + jnp.where(place_t[0] >= 1, pltpu.roll(high, 1, 0), 0.0)
            rim[c, DEG] = high + jnp.where(place_t[0] < half - 1, pltpu.roll(low, 2 * half - 1, 0), 0.0)
            send_x[slot, 0, c] = rim[c, :, 0:half, :]
            send_x[slot, 1, c] = rim[c, :, half : 2 * half, :]
            for a in range(2):
                for b in range(2):
                    at = a * half + b * (half - 1)
                    send_c[slot, 2 * a + b, c] = rim[c, b * DEG, at : at + 1, :]
        start_all(slot, along_x_or_corner)

    def correct(axis, step, slot):
        normal, side = axis, 1 - axis
        beta = coef[1, step]
        plain = coef[2, step]
        edge_z = edge_in[...]
        edge_n = by_side(axis, -edge, edge)
        own_f = by_side(axis, float(np.float32(own[0, 0])), float(np.float32(own[DEG, DEG])))
        second_f = float(np.float32(second[0, 0]))
        per_w = float(np.float32(1.0 / weights[0]))
        chain_f = [sum(derivative[k, f] * weights[k] * own[k, f] for k in range(N1) if k != f) for f in (0, DEG)]
        first_f = by_side(axis, float(np.float32(derivative[0, 0])), float(np.float32(derivative[DEG, DEG])))
        then_f = by_side(axis, *(float(np.float32(-value)) for value in chain_f))
        size = 2 * per_side[axis]
        half = per_side[0]
        d = [[None] * N1 for _ in range(3)]
        for c in range(3):
            for t in range(N1):
                value = (plain + beta * scale[axis][c, t]) * arrived[axis][c, t]
                if axis == 1 and t in (0, DEG):
                    value = jnp.where(place_t[1] == (0 if t == 0 else last_x), 0.0, value)
                d[c][t] = value
        d_n, d_t, d_z = d[normal], d[side], d[2]

        def stack(lines):
            return jnp.concatenate(lines, axis=0)

        def joint(parts, matrix, count):
            both = jnp.dot(
                jnp.concatenate(parts, axis=1), matrix[...], preferred_element_type=jnp.float32
            )
            return (both[:, :128] + both[:, 128:]).reshape(count, N1, size, 128)

        g_z = joint(halves(stack(d_z)), own_mat, 1)[0]
        g_t = apply_pairs(own, d_t, -1)
        second_n = apply_pairs(second, d_n, 1)
        second_z = apply_pairs(second, d_z, 1)
        t_n, t_t, t_z, left, v_n, v_t, extra, f_z = [[] for _ in range(8)]
        stiff, mixed, mixed_t, mixed_z, one_t, one_z = [[] for _ in range(6)]
        for t in range(N1):
            lam = face_w[axis, 0, t]
            mu = face_w[axis, 1, t]
            g_n = own_f * d_n[t]
            g_nt = g_n + g_t[t]
            e_n = edge_n * d_n[t]
            e_z = edge_z * d_z[t]
            away_z = g_z[t] - e_z
            shrink = (g_nt + away_z) - e_n
            own_t = g_t[t]
            right = second_f * d_t[t]
            mu_d = mu * d_n[t]
            mu_in = per_w * mu_d
            mixed.append(per_w * (lam * d_n[t]) + mu_in)
            stiff.append(mixed[t] + mu_in)
            if t in (0, DEG):
                edge_t = -edge if t == 0 else edge
                e_t = edge_t * d_t[t]
                shrink = shrink - e_t
                own_t = own_t - (e_t + e_t)
                right = right + edge_t * (g_n + g_z[t])
                mixed_t.append(edge_t * mu_in)
            else:
                mixed_t.append(None)
            base = lam * shrink + mu * (g_nt + g_z[t])
            t_n.append(base + mu * (g_n - (e_n + e_n)))
            t_t.append(base + mu * own_t)
            t_z.append(base + mu * (away_z - e_z))
            left.append(mu * (second_n[t] + edge_n * (g_t[t] + g_z[t])))
            v_n.append(mu_d)
            v_t.append(mu * d_t[t])
            extra.append(mu * right)
            f_z.append(mu * ((second_f * d_z[t] + second_z[t]) + edge_z * g_nt))
            mixed_z.append(edge_z * mu_in)
            one_t.append(per_w * v_t[t])
            one_z.append(per_w * (mu * d_z[t]))
        back_t = apply_pairs(-derivative.T, t_t, -1)
        back_m = apply_pairs(-derivative.T, mixed, -1)
        f_t = [back_t[t] + extra[t] for t in range(N1)]
        two_t = [back_m[t] if mixed_t[t] is None else back_m[t] + mixed_t[t] for t in range(N1)]
        parts = halves(stack(left + f_t)) + halves(stack(v_n + v_t))
        faces = joint(parts, second_mat, 2)
        parts = halves(stack(f_z)) + halves(stack(t_z))
        face_z = joint(parts, back_mat, 1)[0]

        def joined(lines, count):
            return jnp.dot(
                jnp.concatenate(halves(stack(lines)), axis=1),
                exact_mat[...],
                preferred_element_type=jnp.float32,
            ).reshape(count, N1, size, 128)

        along_n = joined(t_n + stiff, 2)
        away = joined(one_t + two_t + one_z, 3)
        parts = halves(stack(mixed_z)) + halves(stack(mixed))
        upright = joint(parts, back_mat, 1)[0]
        at_face = {normal: faces[0], side: faces[1], 2: face_z}
        if axis == 0:
            for c in range(3):
                gather_x(resid, c, 0, DEG, rim, c)
        for c in range(3):
            for t in range(N1):
                value = at_face[c][t]
                if c == normal:
                    value = value + (then_f * along_n[1, t] - first_f * along_n[0, t])
                if axis == 0:
                    left_over = rim[c, t] - value
                    rim[c, t] = left_over
                    delta[c, t] = left_over
                else:
                    add_y(resid, c, t, -value)
        if axis == 0:
            for c in range(3):
                for t in range(N1):
                    resid[c, 0, t, lines_low, :] = delta[c, t, 0:half, :]
                    resid[c, DEG, t, lines_high, :] = delta[c, t, half : 2 * half, :]
            send_rim(slot)
        pairs = {normal: (0, -along_n[0], along_n[1]), side: (2, away[0], away[1]), 2: (2, away[2], upright)}
        for c in range(3):
            for t in range(N1):
                if axis == 0:
                    delta[c, t] = d[c][t]
                    add_x(field, c, t)
                    add_x(change, c, t)
                else:
                    add_y(field, c, t, d[c][t])
                    add_y(change, c, t, d[c][t])
        for t in range(N1):
            for c in range(3):
                kind, first, then = pairs[c]
                if axis == 0:
                    for k, value in enumerate((first[t], then[t])):
                        narrow[2 * c + k, t] = value
                        wide[2 * c + k, t, lines_low, :] = narrow[2 * c + k, t, 0:half, :]
                        wide[2 * c + k, t, lines_high, :] = narrow[2 * c + k, t, half : 2 * half, :]
                    first_t, then_t = wide[2 * c, t], wide[2 * c + 1, t]
                    for p in range(N1):
                        change_by = rank_x[kind, p] * first_t + rank_x[kind + 1, p] * then_t
                        resid[c, p, t] = resid[c, p, t] - change_by
                else:
                    for p in range(N1):
                        for w, rows in enumerate(windows):
                            change_by = rank_y[w, kind, p] * first[t] + rank_y[w, kind + 1, p] * then[t]
                            resid[c, t, p, rows] = resid[c, t, p, rows] - change_by

    for c in range(3):
        fill(field, 0, c)

    pl.semaphore_wait(barrier, len(partners))

    start_all(0, every)

    @pl.loop(0, 3)
    def _(c):
        loads.wait_part(1, c)
        enter(source_in, source, c)

    rank_tables()
    face_weights()
    for ref in (scale_x, scale_y, wide):
        ref[...] = jnp.zeros(ref.shape, jnp.float32)

    for c in range(3):

        @pl.loop(0, N1)
        def _(i):
            change[c, i] = zeros_big
            resid[c, i] = zeros_big

    for c in range(3):
        fill(inverse, 2, c)

    start_all(2, every)

    @pl.loop(0, steps + 1)
    def _(step):
        slot = step % 2
        volume(step, slot)
        arrive_y(slot)
        correct(1, step, 1 - slot)
        wait_for(slot, along_x_or_corner)
        arrive_x(slot)
        correct(0, step, 1 - slot)

        @pl.loop(0, 3)
        def _(c):
            local_sum(resid, c)
            fill_y(resid, 1 - slot, c)

        start_all(1 - slot, along_y)

        @pl.when(step == 0)
        def _():
            wait_for(2, every)

            @pl.loop(0, 3)
            def _(c):
                collect(inverse, 2, c)

                @pl.loop(0, N1)
                def _(i):
                    inverse[c, i] = 1.0 / inverse[c, i]

            face_scales()

    @pl.loop(0, 3)
    def _(c):
        leave(field, smoothed_out, c)

    @pl.loop(0, 3)
    def _(c):
        leave(resid, residual_out, c)

    edge_lines[...] = jnp.zeros(edge_lines.shape, jnp.float32)
    slot = (steps + 1) % 2
    wait_for(slot, every)
    arrive_y(slot)
    arrive_x(slot)
    for c in range(3):
        for t in range(DEG):
            edge_lines[c, 0, pl.ds(t, elems_y, stride=DEG), :] = arrived_x[c, t, 0:elems_y, :]
            edge_lines[c, 1, pl.ds(t, elems_x, stride=DEG), :] = arrived_y[c, t, 0:elems_x, :]
        edge_lines[c, 1, 0:1, :] = jnp.zeros((1, 128), jnp.float32)
    depth = edge_lines.shape[2]
    parts = halves(edge_lines[...].reshape(6 * depth, 128))
    found = jnp.dot(
        jnp.concatenate(parts, axis=1), select_in[...], preferred_element_type=jnp.float32
    )
    patch_out[...] = found.reshape(patch_out.shape)


def finish(nodes_z, nodes_x, nodes_y, smoothed_in, residual_in, patch_in, smoothed_out, residual_out, held, put_sem):
    def put(at, source, target, c):
        return pltpu.make_async_copy(source.at[c], target.at[c], put_sem.at[at, c])

    for c in range(3):
        put(0, smoothed_in, smoothed_out, c).start()
    for c in range(3):
        pieces = [patch_in[c, 0, y : y + 1, 0:nodes_z] for y in range(nodes_y)]
        held[c] = residual_in[c]
        held[c, 0:1, :] = held[c, 0:1, :] + jnp.concatenate(pieces, axis=1)
        held[c, :, 0:nodes_z] = held[c, :, 0:nodes_z] + patch_in[c, 1, 0:nodes_x, 0:nodes_z]
        put(1, held, residual_out, c).start()
    for c in range(3):
        put(0, smoothed_in, smoothed_out, c).wait()
        put(1, held, residual_out, c).wait()


def z_join(blocks, clamped):
    nodes = DEG * blocks + 1
    gather = np.zeros((nodes, blocks * N1))
    for element in range(blocks):
        for k in range(N1):
            gather[DEG * element + k, element * N1 + k] = 1.0
    if clamped:
        gather[0] = 0.0
        gather[nodes - 1] = 0.0
    return gather.T @ gather


def local(right_side, guess, material, lame, upper, lower_ratio):
    elems_x, elems_y, elems_z = material.shape
    cols = elems_x * elems_y
    lanes = N1 * elems_z
    nodes_z = DEG * elems_z - 1
    weights_np, derivative_np, ratio_np, own_np_1, second_np = element_tables()
    eye_z = np.eye(elems_z)
    join_np = z_join(elems_z, True)
    joined = join_np.astype(jnp.bfloat16)

    def exact_pair(matrix):
        high, low = np_halves(matrix)
        none = np.zeros_like(high)
        return [[high, low], [high, none]]

    exact_join = [[joined, np.zeros_like(joined)]] * 2
    own_mat = jnp.asarray(np.block(exact_pair(np.kron(eye_z, own_np_1.T))))
    back_np = np.kron(eye_z, derivative_np) @ join_np
    back_mat = jnp.asarray(np.block(exact_join + exact_pair(-back_np)))
    scaled_np = np.kron(eye_z, second_np) @ join_np
    second_mat = jnp.asarray(np.block(exact_join + exact_pair(scaled_np)))
    exact_mat = jnp.asarray(np.concatenate([joined, joined], axis=0))
    edge_np = np.zeros((1, lanes))
    edge_np[0, 0::N1] = -1.0 / weights_np[0]
    edge_np[0, DEG::N1] = 1.0 / weights_np[DEG]
    edge_in = jnp.asarray(edge_np, jnp.float32)
    all_join = z_join(elems_z, False).astype(jnp.bfloat16)
    join_in = jnp.asarray(np.concatenate([all_join, all_join], axis=0))

    weights_z = np.tile(weights_np, elems_z)
    ratio_z = np.tile(ratio_np, elems_z)
    weight_np = weights_np[:, None, None] * weights_np[None, :, None] * weights_z
    shape_w = (N1, N1, lanes)
    own_x = np.broadcast_to(ratio_np[:, None, None], shape_w)
    own_y = np.broadcast_to(ratio_np[None, :, None], shape_w)
    own_z = np.broadcast_to(ratio_z, shape_w)
    own_np = np.stack([own_x, own_y, own_z])
    weight_in = jnp.asarray(weight_np[:, :, None], jnp.float32)
    own_in = jnp.asarray(own_np[:, :, :, None], jnp.float32)
    sum_in = jnp.asarray((own_x + own_y + own_z)[:, :, None], jnp.float32)

    gather_np = clamped_gather(elems_z)
    nodes_z = gather_np.shape[0]
    owned_np = gather_np.copy()
    owned_np[:, DEG::N1] = 0.0
    enter_np = np.zeros((lanes, lanes))
    enter_np[:nodes_z] = gather_np
    leave_np = np.zeros((lanes, lanes))
    leave_np[:, :nodes_z] = owned_np.T
    gather_in = jnp.asarray(np.concatenate([enter_np, enter_np], axis=0).astype(jnp.bfloat16))
    select_in = jnp.asarray(np.concatenate([leave_np, leave_np], axis=0).astype(jnp.bfloat16))
    spread_in = jnp.asarray(np.kron(eye_z, np.ones((1, N1))), dtype=jnp.float32)

    pad_x = -(-DEG * elems_x // 8) * 8
    whole = (3, N1, N1, cols, lanes)
    smem = pl.BlockSpec(memory_space=pltpu.SMEM)
    big = pltpu.VMEM(whole, jnp.float32)
    small = pltpu.VMEM((N1, N1, cols, lanes), jnp.float32)
    ring = 2 * elems_x
    face_a = pltpu.VMEM((3, N1, 2 * elems_y, lanes), jnp.float32)
    face_b = pltpu.VMEM((3, N1, ring, lanes), jnp.float32)
    edge_size = -(-DEG * max(elems_x, elems_y) // 8) * 8
    lines = pltpu.VMEM((DEG * elems_y, pad_x, lanes), jnp.float32)
    face_x = pltpu.VMEM((SLOTS, 2, 3, N1, elems_y, lanes), jnp.float32)
    face_y = pltpu.VMEM((SLOTS, 2, 3, N1, elems_x, lanes), jnp.float32)
    corner = pltpu.VMEM((SLOTS, 4, 3, 1, lanes), jnp.float32)
    shape = jax.ShapeDtypeStruct(guess.shape, jnp.float32)

    operands = [
        guess,
        right_side,
        material,
        weight_in,
        own_in,
        sum_in,
        spread_in,
        gather_in,
        select_in,
        edge_in,
        own_mat,
        back_mat,
        second_mat,
        exact_mat,
        join_in,
    ]
    number = len(operands)

    def kernel(*refs):
        scalars, places, outs = refs[:3], refs[3 : 3 + number], refs[3 + number : 6 + number]
        staged, rest = refs[6 + number : 6 + 2 * number], refs[6 + 2 * number :]
        loads = Loads(places, staged, *rest[:2])
        smoother_kernel(SWEEPS * CHEB, elems_x, elems_y, *scalars, loads, *outs, *rest[2:])

    away = pl.BlockSpec(memory_space=pl.ANY)
    vmem = pl.BlockSpec(memory_space=pltpu.VMEM)
    operands = [pltpu.with_memory_space_constraint(operand, pltpu.HBM) for operand in operands]
    patch_shape = (3, 2, edge_size, lanes)
    results = pl.pallas_call(
        kernel,
        out_shape=(shape, shape, jax.ShapeDtypeStruct(patch_shape, jnp.float32)),
        in_specs=[smem] * 3 + [away] * number,
        out_specs=(vmem, vmem, vmem),
        scratch_shapes=[pltpu.VMEM(operand.shape, operand.dtype) for operand in operands]
        + [pltpu.SemaphoreType.DMA((2, 3)), pltpu.SemaphoreType.DMA((number,))]
        + [pltpu.VMEM((3, SWEEPS * CHEB + 1, 1, lanes), jnp.float32)]
        + [big] * 3
        + [small] * 2
        + [big] * 3
        + [small] * 3
        + [face_a, face_b] * 2
        + [pltpu.VMEM((4, N1, cols, lanes), jnp.float32)]
        + [pltpu.VMEM((2, 4, N1, ring, lanes), jnp.float32)]
        + [face_a] * 2
        + [pltpu.VMEM((6, N1, 2 * elems_y, lanes), jnp.float32)]
        + [pltpu.VMEM((6, N1, cols, lanes), jnp.float32)]
        + [pltpu.VMEM((2, 2, N1, ring, lanes), jnp.float32)]
        + [pltpu.VMEM(patch_shape, jnp.float32)]
        + [lines] * 2
        + [face_x, face_y, corner] * 2
        + [pltpu.SemaphoreType.DMA((SLOTS, 8))] * 2,
        compiler_params=pltpu.CompilerParams(
            collective_id=0, has_side_effects=True, vmem_limit_bytes=VMEM_BYTES
        ),
    )(pltpu.with_memory_space_constraint(lame, pltpu.HBM), upper, lower_ratio, *operands)

    def finish_kernel(*refs):
        finish(nodes_z, DEG * elems_x, DEG * elems_y, *refs)

    return pl.pallas_call(
        finish_kernel,
        out_shape=(shape, shape),
        in_specs=[vmem] * 3,
        out_specs=(away, away),
        scratch_shapes=[pltpu.VMEM(guess.shape, jnp.float32), pltpu.SemaphoreType.DMA((2, 3))],
        compiler_params=pltpu.CompilerParams(vmem_limit_bytes=VMEM_BYTES // 2),
    )(*results)


def solution(mesh):
    placed = (P(None, "gx", "gy"), P(None, "gx", "gy"), P("gx", "gy", None), P(), P(), P())
    return jax.shard_map(
        local,
        mesh=mesh,
        in_specs=placed,
        out_specs=(P(None, "gx", "gy"), P(None, "gx", "gy")),
        check_vma=False,
    )
```
